8 devices in a mesh: data: 1 (over z), hid: 2 (over y), vocab: 4 (over x, core).
Axes of the slice: x: 2, y: 2, z: 1, core: 2. Of those that a mesh axis runs over, the one named last changes fastest.
Arguments:
- h_states: bfloat16 [1024, 5120], P('data', 'hid')
- w_head: bfloat16 [5120, 100352], P('hid', 'vocab')
- inv_temp: float32 [1024], P('data')
- tgt_ids: int32 [1024], P('data')
Outputs:
- output 1: float32 [1024, 100352], P('data', ('vocab', 'hid'))
- output 2: float32 [1024], P('data')
All inputs are finite; a program needn't handle non-finite values.
Results may differ from the reference program's by a relative error of at most 0.001.
Values are sent between devices in bfloat16 or wider.
A program may use at most 1 GiB of HBM per device.

```python
import jax
import jax.numpy as jnp
from jax import lax
import math

B = 1024
D = 5120
V = 100352


def setup_inputs(seed: int = 0, part: int = 0) -> dict:
    part_keys = jax.random.split(jax.random.fold_in(jax.random.key(seed), part), 5)
    shared_keys = jax.random.split(jax.random.key(seed + 1), 2)
    common_dir = jax.random.normal(shared_keys[0], (D,), jnp.float32)
    col_level = 140.0 - 2.5 * jnp.arange(V, dtype=jnp.float32) / V
    row_keys = jax.random.split(shared_keys[1], D // 128)
    dir_blocks = common_dir.reshape(D // 128, 128)

    def weight_block(block_args):
        blk_key, dir_part = block_args
        noise_blk = jax.random.normal(blk_key, (128, V), jnp.float32)
        w_part = noise_blk * (0.6 / math.sqrt(D)) + dir_part[:, None] * (col_level[None, :] / D)
        return w_part.astype(jnp.bfloat16)

    w_head = lax.map(weight_block, (row_keys, dir_blocks)).reshape(D, V)
    row_noise = jax.random.normal(part_keys[0], (B, D), jnp.float32)
    row_shift = jax.random.uniform(part_keys[1], (B,), jnp.float32, 1.0, 2.0)
    h_states = (row_noise + row_shift[:, None] * common_dir[None, :]).astype(jnp.bfloat16)
    inv_temp = jax.random.uniform(part_keys[2], (B,), jnp.float32, 0.7, 1.3)
    first_pick = jax.random.randint(part_keys[3], (B,), 0, V)
    second_pick = jax.random.randint(part_keys[4], (B,), 0, V)
    tgt_ids = jnp.maximum(first_pick, second_pick).at[0].set(0).at[1].set(V - 1)
    return {"h_states": h_states, "w_head": w_head, "inv_temp": inv_temp, "tgt_ids": tgt_ids}


def reference(h_states, w_head, inv_temp, tgt_ids):
    logits = jnp.dot(h_states, w_head, preferred_element_type=jnp.float32) * inv_temp[:, None]
    row_max = jnp.max(logits, axis=1, keepdims=True)
    exp_vals = jnp.exp(logits - row_max)
    row_sum = jnp.sum(exp_vals, axis=1, keepdims=True)
    prob_rows = exp_vals / row_sum
    cdf_table = jnp.cumsum(prob_rows, axis=1)
    cdf_at_tgt = jnp.take_along_axis(cdf_table, tgt_ids[:, None], axis=1)[:, 0]
    return (cdf_table, cdf_at_tgt)
```

```python
import functools

import jax
import jax.numpy as jnp
from jax import lax
from jax.experimental import pallas as pl
from jax.experimental.pallas import tpu as pltpu
from jax.sharding import PartitionSpec as P


CT = 256
SUB = 32


def mm_kernel(sel_ref, h_ref, w_ref, *out_refs, splits):
    res = jnp.dot(h_ref[...], w_ref[...], preferred_element_type=jnp.float32)
    at = 0
    for ref, rows in zip(out_refs, splits):
        ref[...] = res[at:at + rows]
        at += rows


def partial_products(h, w, half, row0, splits, tile0, ntiles, tn, half_tiles, name):
    rows = sum(splits)
    depth = h.shape[1]
    cols = ntiles * tn
    return pl.pallas_call(
        functools.partial(mm_kernel, splits=splits),
        out_shape=[jax.ShapeDtypeStruct((r, cols), jnp.float32) for r in splits],
        grid_spec=pltpu.PrefetchScalarGridSpec(
            num_scalar_prefetch=1,
            grid=(ntiles,),
            in_specs=[
                pl.BlockSpec((rows, depth), lambda j, s: (row0 // rows, 0)),
                pl.BlockSpec((depth, tn), lambda j, s: (0, s[0] * half_tiles + tile0 + j)),
            ],
            out_specs=[pl.BlockSpec((r, tn), lambda j, s: (0, j)) for r in splits],
        ),
        cost_estimate=pl.CostEstimate(
            flops=2 * rows * depth * cols, bytes_accessed=depth * cols * 2 + rows * cols * 4, transcendentals=0),
        compiler_params=pltpu.CompilerParams(
            dimension_semantics=("arbitrary",), vmem_limit_bytes=48 * 1024 * 1024),
        name=name,
    )(half, h, w)


def local_kernel(temp_ref, tgt_ref, tri_ref, own_ref, *refs, npieces):
    recv_refs = refs[:npieces]
    pre_ref, st_ref, z_s, hi_s, mid_s, lo_s = refs[npieces:]
    rows = own_ref.shape[0]
    nt = own_ref.shape[1] // CT
    temp = jnp.broadcast_to(temp_ref[...], (rows, CT))
    mx = jnp.full((rows, CT), -jnp.inf, jnp.float32)
    t0 = 0
    for ref in recv_refs:
        n = ref.shape[1] // CT

        def max_step(j, mx, ref=ref, t0=t0):
            src = pl.ds(pl.multiple_of(j * CT, CT), CT)
            dst = pl.ds(pl.multiple_of((t0 + j) * CT, CT), CT)
            z = (own_ref[:, dst] + ref[:, src]) * temp
            z_s[t0 + j] = z
            return jnp.maximum(mx, z)

        mx = lax.fori_loop(0, n, max_step, mx, unroll=7)
        t0 += n
    m = jnp.max(mx, axis=1, keepdims=True)
    mb = jnp.broadcast_to(m, (rows, CT))
    tgt = jnp.broadcast_to(tgt_ref[...], (rows, CT))
    col = lax.broadcasted_iota(jnp.int32, (rows, CT), 1)
    rel = tgt - col

    def exp_step(j, carry):
        sacc, cacc = carry
        e = jnp.exp(z_s[j] - mb)
        hi = e.astype(jnp.bfloat16)
        r1 = e - hi.astype(jnp.float32)
        mid = r1.astype(jnp.bfloat16)
        lo = (r1 - mid.astype(jnp.float32)).astype(jnp.bfloat16)
        hi_s[j] = hi
        mid_s[j] = mid
        lo_s[j] = lo
        return sacc + e, cacc + jnp.where(rel >= j * CT, e, 0.0)

    zero = jnp.zeros((rows, CT), jnp.float32)
    sacc, cacc = lax.fori_loop(0, nt, exp_step, (zero, zero), unroll=7)
    s = jnp.sum(sacc, axis=1, keepdims=True)
    c = jnp.sum(cacc, axis=1, keepdims=True)
    lane = lax.broadcasted_iota(jnp.int32, (rows, 128), 1)
    st_ref[...] = jnp.where(lane == 0, m, jnp.where(lane == 1, s, jnp.where(lane == 2, c, 0.0)))

    tri = tri_ref[...]
    group = 7

    def prefix_step(g, carry):
        at = pl.ds(g * group, group)
        pre = jnp.dot(hi_s[at].reshape(group * rows, CT), tri, preferred_element_type=jnp.float32)
        pre += jnp.dot(mid_s[at].reshape(group * rows, CT), tri, preferred_element_type=jnp.float32)
        pre += jnp.dot(lo_s[at].reshape(group * rows, CT), tri, preferred_element_type=jnp.float32)
        for k in range(group):
            blk = pre[k * rows:(k + 1) * rows]
            dst = pl.ds(pl.multiple_of((g * group + k) * CT, CT), CT)
            pre_ref[:, dst] = blk + carry
            carry = carry + jnp.broadcast_to(blk[:, CT - 1:CT], (rows, CT))
        return carry

    lax.fori_loop(0, nt // group, prefix_step, zero)


def local_prefix(temp, tgt, tri, own, own_row0, recvs, rows, row0, name):
    cols = own.shape[1]
    nt = cols // CT
    return pl.pallas_call(
        functools.partial(local_kernel, npieces=len(recvs)),
        grid=(rows // SUB,),
        out_shape=[jax.ShapeDtypeStruct((rows, cols), jnp.float32), jax.ShapeDtypeStruct((rows, 128), jnp.float32)],
        in_specs=[
            pl.BlockSpec((SUB, 1), lambda i: (row0 // SUB + i, 0)),
            pl.BlockSpec((SUB, 1), lambda i: (row0 // SUB + i, 0)),
            pl.BlockSpec((CT, CT), lambda i: (0, 0)),
            pl.BlockSpec((SUB, cols), lambda i: (own_row0 // SUB + i, 0)),
        ] + [pl.BlockSpec((SUB, r.shape[1]), lambda i: (i, 0)) for r in recvs],
        out_specs=[pl.BlockSpec((SUB, cols), lambda i: (i, 0)), pl.BlockSpec((SUB, 128), lambda i: (i, 0))],
        scratch_shapes=[
            pltpu.VMEM((nt, SUB, CT), jnp.float32),
            pltpu.VMEM((nt, SUB, CT), jnp.bfloat16),
            pltpu.VMEM((nt, SUB, CT), jnp.bfloat16),
            pltpu.VMEM((nt, SUB, CT), jnp.bfloat16),
        ],
        cost_estimate=pl.CostEstimate(
            flops=6 * rows * cols * CT, bytes_accessed=rows * cols * 12, transcendentals=rows * cols),
        compiler_params=pltpu.CompilerParams(
            dimension_semantics=("arbitrary",), vmem_limit_bytes=32 * 1024 * 1024),
        name=name,
    )(temp, tgt, tri, own, *recvs)


def final_kernel(pos_ref, pre_ref, mine_ref, other_ref, *refs):
    out_ref, ct_ref = refs[-2:]
    voc, hid = pos_ref[0], pos_ref[1]
    nv = mine_ref.shape[0]
    stats = [(v, mine_ref[v], True) for v in range(nv)] + [(v, other_ref[v], False) for v in range(nv)]
    top = functools.reduce(jnp.maximum, [st[:, 0:1] for _, st, _ in stats])
    total = below = at_tgt = jnp.zeros_like(top)
    scale = None
    for v, st, same in stats:
        f = jnp.exp(st[:, 0:1] - top)
        s = st[:, 1:2] * f
        total += s
        at_tgt += st[:, 2:3] * f
        lower = (v < voc) if same else ((v < voc) | ((v == voc) & (hid == 1)))
        below += jnp.where(lower, s, 0.0)
        if same:
            scale = jnp.where(v == voc, f, 0.0) if scale is None else jnp.where(v == voc, f, scale)
    inv = 1.0 / total
    ct_ref[...] = jnp.broadcast_to(at_tgt * inv, ct_ref.shape)
    out_ref[...] = pre_ref[...] * (scale * inv) + below * inv


def finish(pos, pre, mine, other, out, all_rows, row0, name):
    rows, cols = pre.shape
    nv = mine.shape[0]
    ins = [pos, pre, mine, other]
    in_specs = [
        pl.BlockSpec((SUB, cols), lambda i, s: (i, 0)),
        pl.BlockSpec((nv, SUB, 128), lambda i, s: (0, i, 0)),
        pl.BlockSpec((nv, SUB, 128), lambda i, s: (0, i, 0)),
    ]
    aliases = {}
    if out is not None:
        ins.append(out)
        in_specs.append(pl.BlockSpec(memory_space=pl.ANY))
        aliases = {4: 0}
    return pl.pallas_call(
        final_kernel,
        out_shape=[jax.ShapeDtypeStruct((all_rows, cols), jnp.float32), jax.ShapeDtypeStruct((rows, 128), jnp.float32)],
        grid_spec=pltpu.PrefetchScalarGridSpec(
            num_scalar_prefetch=1,
            grid=(rows // SUB,),
            in_specs=in_specs,
            out_specs=[pl.BlockSpec((SUB, cols), lambda i, s: (row0 // SUB + i, 0)),
                       pl.BlockSpec((SUB, 128), lambda i, s: (i, 0))],
        ),
        input_output_aliases=aliases,
        cost_estimate=pl.CostEstimate(flops=64 * rows * cols, bytes_accessed=rows * cols * 8, transcendentals=0),
        compiler_params=pltpu.CompilerParams(
            dimension_semantics=("arbitrary",), vmem_limit_bytes=32 * 1024 * 1024),
        name=name,
    )(*ins)


def solution(mesh):
    def local_step(h, w, temp, tgt):
        rows_all = h.shape[0]
        cols = w.shape[1] // 2
        hid = lax.axis_index("hid")
        voc = lax.axis_index("vocab")
        own_half = hid.astype(jnp.int32).reshape(1)
        peer_half = (1 - hid).astype(jnp.int32).reshape(1)
        pos = jnp.stack([voc, hid]).astype(jnp.int32)
        temp2 = temp[:, None]
        tgt2 = (tgt - (voc * 2 + hid) * cols)[:, None]
        tri = (lax.broadcasted_iota(jnp.int32, (CT, CT), 0) <= lax.broadcasted_iota(jnp.int32, (CT, CT), 1)).astype(jnp.bfloat16)
        swap = [(0, 1), (1, 0)]

        blk = 128
        nblk = rows_all // blk
        tail = (64, 32, 32)
        tn = 7 * CT
        ht = cols // tn
        units = []
        owns = []
        for b in range(nblk):
            if b == 0:
                first = partial_products(h, w, peer_half, 0, (blk,), 0, 7, CT, cols // CT, "mm_peer0a")
                rest = partial_products(h, w, peer_half, 0, (blk,), 1, ht - 1, tn, ht, "mm_peer0b")
                units.append((b, 0, blk, [first[0], rest[0]]))
            else:
                splits = tail if b == nblk - 1 else (blk,)
                outs = partial_products(h, w, peer_half, b * blk, splits, 0, ht, tn, ht, f"mm_peer{b}")
                at = 0
                for o, r in zip(outs, splits):
                    units.append((b, at, r, [o]))
                    at += r
            owns.append(partial_products(h, w, own_half, b * blk, (blk,), 0, ht, tn, ht, f"mm_own{b}")[0])

        out = None
        at_tgt = []
        mine = []
        pend = []
        for k, (b, at, rows, pieces) in enumerate(units):
            if k >= 2:
                *pieces, mine[k - 2] = lax.optimization_barrier((*pieces, mine[k - 2]))
                pend.append((k - 2, lax.ppermute(mine[k - 2], "hid", swap)))
            recvs = [lax.ppermute(p, "hid", swap) for p in pieces]
            pre, st = local_prefix(temp2, tgt2, tri, owns[b], at, recvs, rows, b * blk + at, f"local{k}")
            mine.append(lax.all_gather(st, "vocab"))
            units[k] = units[k] + (pre,)
        others = dict(pend)
        for k in range(len(units)):
            if k not in others:
                others[k] = lax.ppermute(mine[k], "hid", swap)
        for k, (b, at, rows, _, pre) in enumerate(units):
            out, ct = finish(pos, pre, mine[k], others[k], out, rows_all, b * blk + at, f"finish{k}")
            at_tgt.append(ct[:, 0])
        return out, jnp.concatenate(at_tgt)

    return jax.shard_map(
        local_step,
        mesh=mesh,
        in_specs=(P("data", "hid"), P("hid", "vocab"), P("data"), P("data")),
        out_specs=(P("data", ("vocab", "hid")), P("data")),
        check_vma=False,
    )
```

```python
import functools

import jax
import jax.numpy as jnp
from jax import lax
from jax.experimental import pallas as pl
from jax.experimental.pallas import tpu as pltpu
from jax.sharding import PartitionSpec as P


CT = 256
SUB = 32
LAST_VMEM = 32 * 1024 * 1024
ALL_VMEM = 67043328


def mm_kernel(sel_ref, h_ref, w_ref, *refs, splits):
    out_refs = refs[len(refs) - len(splits):]
    res = jnp.dot(h_ref[...], w_ref[...], preferred_element_type=jnp.float32)
    at = 0
    for ref, rows in zip(out_refs, splits):
        ref[...] = res[at:at + rows]
        at += rows


def partial_products(h, w, half, row0, splits, tile0, ntiles, tn, half_tiles, deps=()):
    rows = sum(splits)
    depth = h.shape[1]
    cols = ntiles * tn
    return pl.pallas_call(
        functools.partial(mm_kernel, splits=splits),
        out_shape=[jax.ShapeDtypeStruct((r, cols), jnp.float32) for r in splits],
        grid_spec=pltpu.PrefetchScalarGridSpec(
            num_scalar_prefetch=1,
            grid=(ntiles,),
            in_specs=[
                pl.BlockSpec((rows, depth), lambda j, s: (row0 // rows, 0)),
                pl.BlockSpec((depth, tn), lambda j, s: (0, s[0] * half_tiles + tile0 + j)),
            ] + [pl.BlockSpec(memory_space=pl.ANY)] * len(deps),
            out_specs=[pl.BlockSpec((r, tn), lambda j, s: (0, j)) for r in splits],
        ),
        cost_estimate=pl.CostEstimate(
            flops=2 * rows * depth * cols, bytes_accessed=depth * cols * 2 + rows * cols * 4, transcendentals=0),
        compiler_params=pltpu.CompilerParams(dimension_semantics=("arbitrary",), vmem_limit_bytes=ALL_VMEM),
    )(half, h, w, *deps)


def local_kernel(temp_ref, tgt_ref, tri_ref, own_ref, *refs, npieces, ndeps):
    recv_refs = refs[:npieces]
    pre_ref, st_ref, z_s, hi_s, mid_s, lo_s = refs[npieces + ndeps:]
    rows = own_ref.shape[0]
    nt = own_ref.shape[1] // CT
    temp = jnp.broadcast_to(temp_ref[...], (rows, CT))
    mx = jnp.full((rows, CT), -jnp.inf, jnp.float32)
    t0 = 0
    for ref in recv_refs:
        n = ref.shape[1] // CT

        def max_step(j, mx, ref=ref, t0=t0):
            src = pl.ds(pl.multiple_of(j * CT, CT), CT)
            dst = pl.ds(pl.multiple_of((t0 + j) * CT, CT), CT)
            z = (own_ref[:, dst] + ref[:, src]) * temp
            z_s[t0 + j] = z
            return jnp.maximum(mx, z)

        mx = lax.fori_loop(0, n, max_step, mx, unroll=7)
        t0 += n
    m = jnp.max(mx, axis=1, keepdims=True)
    mb = jnp.broadcast_to(m, (rows, CT))
    tgt = jnp.broadcast_to(tgt_ref[...], (rows, CT))
    col = lax.broadcasted_iota(jnp.int32, (rows, CT), 1)
    rel = tgt - col

    def exp_step(j, carry):
        sacc, cacc = carry
        e = jnp.exp(z_s[j] - mb)
        hi = e.astype(jnp.bfloat16)
        r1 = e - hi.astype(jnp.float32)
        mid = r1.astype(jnp.bfloat16)
        lo = (r1 - mid.astype(jnp.float32)).astype(jnp.bfloat16)
        hi_s[j] = hi
        mid_s[j] = mid
        lo_s[j] = lo
        return sacc + e, cacc + jnp.where(rel >= j * CT, e, 0.0)

    zero = jnp.zeros((rows, CT), jnp.float32)
    sacc, cacc = lax.fori_loop(0, nt, exp_step, (zero, zero), unroll=7)
    s = jnp.sum(sacc, axis=1, keepdims=True)
    c = jnp.sum(cacc, axis=1, keepdims=True)
    lane = lax.broadcasted_iota(jnp.int32, (rows, 128), 1)
    st_ref[...] = jnp.where(lane == 0, m, jnp.where(lane == 1, s, jnp.where(lane == 2, c, 0.0)))

    tri = tri_ref[...]
    group = 7

    def prefix_step(g, carry):
        at = pl.ds(g * group, group)
        pre = jnp.dot(hi_s[at].reshape(group * rows, CT), tri, preferred_element_type=jnp.float32)
        pre += jnp.dot(mid_s[at].reshape(group * rows, CT), tri, preferred_element_type=jnp.float32)
        pre += jnp.dot(lo_s[at].reshape(group * rows, CT), tri, preferred_element_type=jnp.float32)
        for k in range(group):
            blk = pre[k * rows:(k + 1) * rows]
            dst = pl.ds(pl.multiple_of((g * group + k) * CT, CT), CT)
            pre_ref[:, dst] = blk + carry
            carry = carry + jnp.broadcast_to(blk[:, CT - 1:CT], (rows, CT))
        return carry

    lax.fori_loop(0, nt // group, prefix_step, zero)


def local_prefix(temp, tgt, tri, own, own_row0, recvs, rows, row0, deps=(), vmem=ALL_VMEM):
    cols = own.shape[1]
    nt = cols // CT
    sub = min(SUB, rows)
    return pl.pallas_call(
        functools.partial(local_kernel, npieces=len(recvs), ndeps=len(deps)),
        grid=(rows // sub,),
        out_shape=[jax.ShapeDtypeStruct((rows, cols), jnp.float32), jax.ShapeDtypeStruct((rows, 128), jnp.float32)],
        in_specs=[
            pl.BlockSpec((sub, 1), lambda i: (row0 // sub + i, 0)),
            pl.BlockSpec((sub, 1), lambda i: (row0 // sub + i, 0)),
            pl.BlockSpec((CT, CT), lambda i: (0, 0)),
            pl.BlockSpec((sub, cols), lambda i: (own_row0 // sub + i, 0)),
        ] + [pl.BlockSpec((sub, r.shape[1]), lambda i: (i, 0)) for r in recvs]
        + [pl.BlockSpec(memory_space=pl.ANY)] * len(deps),
        out_specs=[pl.BlockSpec((sub, cols), lambda i: (i, 0)), pl.BlockSpec((sub, 128), lambda i: (i, 0))],
        scratch_shapes=[
            pltpu.VMEM((nt, sub, CT), jnp.float32),
            pltpu.VMEM((nt, sub, CT), jnp.bfloat16),
            pltpu.VMEM((nt, sub, CT), jnp.bfloat16),
            pltpu.VMEM((nt, sub, CT), jnp.bfloat16),
        ],
        cost_estimate=pl.CostEstimate(
            flops=6 * rows * cols * CT, bytes_accessed=rows * cols * 12, transcendentals=rows * cols),
        compiler_params=pltpu.CompilerParams(dimension_semantics=("arbitrary",), vmem_limit_bytes=vmem),
    )(temp, tgt, tri, own, *recvs, *deps)


def final_kernel(pos_ref, pre_ref, mine_ref, other_ref, *refs):
    out_ref, ct_ref = refs[-2:]
    voc, hid = pos_ref[0], pos_ref[1]
    nv = mine_ref.shape[0]
    stats = [(v, mine_ref[v], True) for v in range(nv)] + [(v, other_ref[v], False) for v in range(nv)]
    top = functools.reduce(jnp.maximum, [st[:, 0:1] for _, st, _ in stats])
    total = below = at_tgt = scale = jnp.zeros_like(top)
    for v, st, same in stats:
        f = jnp.exp(st[:, 0:1] - top)
        s = st[:, 1:2] * f
        total += s
        at_tgt += st[:, 2:3] * f
        lower = (v < voc) if same else ((v < voc) | ((v == voc) & (hid == 1)))
        below += jnp.where(lower, s, 0.0)
        if same:
            scale = jnp.where(v == voc, f, scale)
    inv = 1.0 / total
    ct_ref[...] = jnp.broadcast_to(at_tgt * inv, ct_ref.shape)
    out_ref[...] = pre_ref[...] * (scale * inv) + below * inv


def last_kernel(pre_ref, ab_ref, *refs):
    out_ref = refs[-1]
    out_ref[...] = pre_ref[...] * ab_ref[:, 0:1] + ab_ref[:, 1:2]


def exchange_kernel(st_ref, ab_ref, slots, send_sem, recv_sem):
    voc = lax.axis_index("vocab")
    hid = lax.axis_index("hid")
    steps = [(dv, dh) for dv in range(4) for dh in range(2)][1:]
    barrier = pltpu.get_barrier_semaphore()
    for dv, dh in steps:
        pl.semaphore_signal(
            barrier, inc=1, device_id={"vocab": lax.rem(voc + dv, 4), "hid": lax.rem(hid + dh, 2)},
            device_id_type=pl.DeviceIdType.MESH)
    pl.semaphore_wait(barrier, len(steps))
    copies = []
    for i, (dv, dh) in enumerate(steps):
        copy = pltpu.make_async_remote_copy(
            src_ref=st_ref,
            dst_ref=slots.at[i],
            send_sem=send_sem.at[i],
            recv_sem=recv_sem.at[i],
            device_id={"vocab": lax.rem(voc + dv, 4), "hid": lax.rem(hid + dh, 2)},
            device_id_type=pl.DeviceIdType.MESH,
        )
        copy.start()
        copies.append(copy)
    for copy in copies:
        copy.wait()
    own = st_ref[...]
    top = own[:, 0:1]
    for i in range(len(steps)):
        top = jnp.maximum(top, slots[i][:, 0:1])
    scale = jnp.exp(own[:, 0:1] - top)
    total = own[:, 1:2] * scale
    at_tgt = own[:, 2:3] * scale
    below = jnp.zeros_like(top)
    for i, (dv, dh) in enumerate(steps):
        st = slots[i]
        f = jnp.exp(st[:, 0:1] - top)
        s = st[:, 1:2] * f
        total += s
        at_tgt += st[:, 2:3] * f
        first = lax.rem(voc + 4 - dv, 4) * 2 + lax.rem(hid + 2 - dh, 2)
        below += jnp.where(first < voc * 2 + hid, s, 0.0)
    inv = 1.0 / total
    lane = lax.broadcasted_iota(jnp.int32, ab_ref.shape, 1)
    ab_ref[...] = jnp.where(lane == 0, scale * inv, jnp.where(lane == 1, below * inv, at_tgt * inv))


def exchange(st):
    rows = st.shape[0]
    return pl.pallas_call(
        exchange_kernel,
        out_shape=jax.ShapeDtypeStruct((rows, 128), jnp.float32),
        in_specs=[pl.BlockSpec(memory_space=pltpu.VMEM)],
        out_specs=pl.BlockSpec(memory_space=pltpu.VMEM),
        scratch_shapes=[
            pltpu.VMEM((7, rows, 128), jnp.float32),
            pltpu.SemaphoreType.DMA((7,)),
            pltpu.SemaphoreType.DMA((7,)),
        ],
        compiler_params=pltpu.CompilerParams(collective_id=0, has_side_effects=True, vmem_limit_bytes=8 * 1024 * 1024),
        name="exchange",
    )(st)


def finish(pos, pre, stats, out, all_rows, row0, name, deps=(), vmem=ALL_VMEM):
    rows, cols = pre.shape
    sub = min(SUB, rows)
    common = dict(
        cost_estimate=pl.CostEstimate(flops=64 * rows * cols, bytes_accessed=rows * cols * 8, transcendentals=0),
        compiler_params=pltpu.CompilerParams(dimension_semantics=("arbitrary",), vmem_limit_bytes=vmem),
        name=name,
    )
    any_spec = pl.BlockSpec(memory_space=pl.ANY)
    tail = ([] if out is None else [out]) + list(deps)
    full = jax.ShapeDtypeStruct((all_rows, cols), jnp.float32)
    if pos is None:
        return pl.pallas_call(
            last_kernel,
            grid=(rows // sub,),
            out_shape=full,
            in_specs=[pl.BlockSpec((sub, cols), lambda i: (i, 0)), pl.BlockSpec((sub, 128), lambda i: (i, 0))]
            + [any_spec] * len(tail),
            out_specs=pl.BlockSpec((sub, cols), lambda i: (row0 // sub + i, 0)),
            input_output_aliases={2: 0},
            **common,
        )(pre, stats, *tail)
    mine, other = stats
    nv = mine.shape[0]
    return pl.pallas_call(
        final_kernel,
        out_shape=[full, jax.ShapeDtypeStruct((rows, 128), jnp.float32)],
        grid_spec=pltpu.PrefetchScalarGridSpec(
            num_scalar_prefetch=1,
            grid=(rows // sub,),
            in_specs=[
                pl.BlockSpec((sub, cols), lambda i, s: (i, 0)),
                pl.BlockSpec((nv, sub, 128), lambda i, s: (0, i, 0)),
                pl.BlockSpec((nv, sub, 128), lambda i, s: (0, i, 0)),
            ] + [any_spec] * len(tail),
            out_specs=[pl.BlockSpec((sub, cols), lambda i, s: (row0 // sub + i, 0)),
                       pl.BlockSpec((sub, 128), lambda i, s: (i, 0))],
        ),
        input_output_aliases={} if out is None else {4: 0},
        **common,
    )(pos, pre, mine, other, *tail)


def solution(mesh):
    def pipeline(h, w, temp, tgt):
        rows_all = h.shape[0]
        cols = w.shape[1] // 2
        hid = lax.axis_index("hid")
        voc = lax.axis_index("vocab")
        own_half = hid.astype(jnp.int32).reshape(1)
        peer_half = (1 - hid).astype(jnp.int32).reshape(1)
        pos = jnp.stack([voc, hid]).astype(jnp.int32)
        temp2 = temp[:, None]
        tgt2 = (tgt - (voc * 2 + hid) * cols)[:, None]
        tri = (lax.broadcasted_iota(jnp.int32, (CT, CT), 0) <= lax.broadcasted_iota(jnp.int32, (CT, CT), 1)).astype(jnp.bfloat16)
        swap = [(0, 1), (1, 0)]

        blk = 128
        nblk = rows_all // blk
        last = (64, 32, 16, 16)
        tn = 7 * CT
        ht = cols // tn

        units = [(b, 0, blk) for b in range(nblk - 1)]
        units += [(nblk - 1, sum(last[:i]), r) for i, r in enumerate(last)]
        nu = len(units)
        parts = {}
        owns = {}
        tok = None

        def peer(b):
            nonlocal tok
            if b >= nblk:
                return
            splits = last if b == nblk - 1 else (blk,)
            outs = partial_products(h, w, peer_half, b * blk, splits, 0, ht, tn, ht, (tok,))
            tok = outs[0]
            for i, o in enumerate(outs):
                parts[b + i] = [o]

        def mine_half(b):
            nonlocal tok
            if b >= nblk:
                return
            tok = owns[b] = partial_products(h, w, own_half, b * blk, (blk,), 0, ht, tn, ht, (tok,))[0]

        tok = partial_products(h, w, peer_half, 0, (blk,), 0, 2, tn // 2, 2 * ht)[0]
        parts[0] = [tok]
        tok = partial_products(h, w, peer_half, 0, (blk,), 1, ht - 1, tn, ht, (tok,))[0]
        parts[0].append(tok)
        peer(1)
        peer(2)
        mine_half(0)
        mine_half(1)

        def send(arrays):
            return [lax.ppermute(a, "hid", swap) for a in arrays]

        recvs = {0: send(parts[0][:1]) + send(parts[0][1:]), 1: send(parts[1])}
        pres, stats, at_tgt = {}, {}, []
        out = None

        def close(k):
            nonlocal out, tok
            b, at, _ = units[k]
            out, ct = finish(pos, pres[k], stats[k], out, rows_all, b * blk + at, f"finish{k}", (tok,))
            at_tgt.append(ct[:, 0])
            tok = ct

        for k, (b, at, rows) in enumerate(units):
            pres[k], st = local_prefix(temp2, tgt2, tri, owns[b], at, recvs[k], rows, b * blk + at, (tok,),
                                        LAST_VMEM if k == nu - 1 else ALL_VMEM)
            if k == nu - 1:
                tok = st
                close(k - 1)
                ab = exchange(st)
                out = finish(None, pres[k], ab, out, rows_all, b * blk + at, f"finish{k}", (tok,), LAST_VMEM)
                at_tgt.append(ab[:, 2])
                break
            mine = lax.all_gather(st, "vocab")
            if k + 2 < nu:
                *sent, mine = lax.optimization_barrier((*parts[k + 2], mine))
                stats[k] = (mine, send([mine])[0])
                recvs[k + 2] = send(sent)
            else:
                stats[k] = (mine, send([mine])[0])
            tok = mine
            if k >= 1:
                close(k - 1)
            peer(k + 3)
            mine_half(k + 2)
        return out, jnp.concatenate(at_tgt)

    return jax.shard_map(
        pipeline,
        mesh=mesh,
        in_specs=(P("data", "hid"), P("hid", "vocab"), P("data"), P("data")),
        out_specs=(P("data", ("vocab", "hid")), P("data")),
        check_vma=False,
    )
```

```python
import functools

import jax
import jax.numpy as jnp
from jax import lax
from jax.experimental import pallas as pl
from jax.experimental.pallas import tpu as pltpu
from jax.sharding import PartitionSpec as P


CT = 256
SUB = 32
ALL_VMEM = 67043328


def mm_kernel(sel_ref, h_ref, w_ref, *refs, splits):
    out_refs = refs[len(refs) - len(splits):]
    res = jnp.dot(h_ref[...], w_ref[...], preferred_element_type=jnp.float32)
    at = 0
    for ref, rows in zip(out_refs, splits):
        ref[...] = res[at:at + rows]
        at += rows


def partial_products(h, w, half, row0, splits, tile0, ntiles, tn, half_tiles, deps=()):
    rows = sum(splits)
    depth = h.shape[1]
    cols = ntiles * tn
    return pl.pallas_call(
        functools.partial(mm_kernel, splits=splits),
        out_shape=[jax.ShapeDtypeStruct((r, cols), jnp.float32) for r in splits],
        grid_spec=pltpu.PrefetchScalarGridSpec(
            num_scalar_prefetch=1,
            grid=(ntiles,),
            in_specs=[
                pl.BlockSpec((rows, depth), lambda j, s: (row0 // rows, 0)),
                pl.BlockSpec((depth, tn), lambda j, s: (0, s[0] * half_tiles + tile0 + j)),
            ] + [pl.BlockSpec(memory_space=pl.ANY)] * len(deps),
            out_specs=[pl.BlockSpec((r, tn), lambda j, s: (0, j)) for r in splits],
        ),
        cost_estimate=pl.CostEstimate(
            flops=2 * rows * depth * cols, bytes_accessed=depth * cols * 2 + rows * cols * 4, transcendentals=0),
        compiler_params=pltpu.CompilerParams(dimension_semantics=("arbitrary",), vmem_limit_bytes=ALL_VMEM),
    )(half, h, w, *deps)


def local_kernel(temp_ref, tgt_ref, tri_ref, own_ref, *refs, npieces, has_prev, skip, at, group):
    recv_refs = refs[:npieces]
    prev_ref = refs[npieces] if has_prev else None
    pre_ref, st_ref, z_s, hi_s, mid_s, lo_s, st_s = refs[npieces + has_prev + skip:]
    step, nsteps = pl.program_id(0), pl.num_programs(0)
    rows = own_ref.shape[0]
    nt = own_ref.shape[1] // CT
    temp = jnp.broadcast_to(temp_ref[...], (rows, CT))
    mx = jnp.full((rows, CT), -jnp.inf, jnp.float32)
    t0 = 0
    for ref in recv_refs:
        n = ref.shape[1] // CT

        def max_step(j, mx, ref=ref, t0=t0):
            src = pl.ds(pl.multiple_of(j * CT, CT), CT)
            dst = pl.ds(pl.multiple_of((t0 + j) * CT, CT), CT)
            z = (own_ref[:, dst] + ref[:, src]) * temp
            z_s[t0 + j] = z
            return jnp.maximum(mx, z)

        mx = lax.fori_loop(0, n, max_step, mx, unroll=7)
        t0 += n
    m = jnp.max(mx, axis=1, keepdims=True)
    mb = jnp.broadcast_to(m, (rows, CT))
    tgt = jnp.broadcast_to(tgt_ref[...], (rows, CT))
    col = lax.broadcasted_iota(jnp.int32, (rows, CT), 1)
    rel = tgt - col

    def exp_step(j, carry):
        sacc, cacc = carry
        e = jnp.exp(z_s[j] - mb)
        hi = e.astype(jnp.bfloat16)
        r1 = e - hi.astype(jnp.float32)
        mid = r1.astype(jnp.bfloat16)
        lo = (r1 - mid.astype(jnp.float32)).astype(jnp.bfloat16)
        hi_s[j] = hi
        mid_s[j] = mid
        lo_s[j] = lo
        return sacc + e, cacc + jnp.where(rel >= j * CT, e, 0.0)

    zero = jnp.zeros((rows, CT), jnp.float32)
    sacc, cacc = lax.fori_loop(0, nt, exp_step, (zero, zero), unroll=7)
    s = jnp.sum(sacc, axis=1, keepdims=True)
    c = jnp.sum(cacc, axis=1, keepdims=True)
    lane = lax.broadcasted_iota(jnp.int32, (rows, 128), 1)

    @pl.when(step == 0)
    def _():
        st_s[...] = jnp.zeros_like(st_s)

    st_s[pl.ds(pl.multiple_of(at + step * rows, rows), rows), :] = jnp.where(
        lane == 0, m, jnp.where(lane == 1, s, jnp.where(lane == 2, c, 0.0)))

    @pl.when(step == nsteps - 1)
    def _():
        st = st_s[...].T[0:8]
        st_ref[...] = st + prev_ref[...] if has_prev else st

    tri = tri_ref[...]

    def prefix_step(g, carry):
        span = pl.ds(g * group, group)
        pre = jnp.dot(hi_s[span].reshape(group * rows, CT), tri, preferred_element_type=jnp.float32)
        pre += jnp.dot(mid_s[span].reshape(group * rows, CT), tri, preferred_element_type=jnp.float32)
        pre += jnp.dot(lo_s[span].reshape(group * rows, CT), tri, preferred_element_type=jnp.float32)
        for k in range(group):
            blk = pre[k * rows:(k + 1) * rows]
            dst = pl.ds(pl.multiple_of((g * group + k) * CT, CT), CT)
            pre_ref[:, dst] = blk + carry
            carry = carry + jnp.broadcast_to(blk[:, CT - 1:CT], (rows, CT))
        return carry

    lax.fori_loop(0, nt // group, prefix_step, zero)


def local_prefix(temp, tgt, tri, own, at, recvs, rows, row0, prev, deps):
    cols = own.shape[1]
    nt = cols // CT
    sub = min(SUB, rows)
    extra = ([] if prev is None else [prev]) + list(deps)
    extra_specs = ([] if prev is None else [pl.BlockSpec((8, 128), lambda i: (0, 0))])
    extra_specs += [pl.BlockSpec(memory_space=pl.ANY)] * len(deps)
    return pl.pallas_call(
        functools.partial(
            local_kernel, npieces=len(recvs), has_prev=int(prev is not None), skip=len(deps), at=at, group=7),
        grid=(rows // sub,),
        out_shape=[jax.ShapeDtypeStruct((rows, cols), jnp.float32), jax.ShapeDtypeStruct((8, 128), jnp.float32)],
        in_specs=[
            pl.BlockSpec((sub, 1), lambda i: (row0 // sub + i, 0)),
            pl.BlockSpec((sub, 1), lambda i: (row0 // sub + i, 0)),
            pl.BlockSpec((CT, CT), lambda i: (0, 0)),
            pl.BlockSpec((sub, cols), lambda i: (at // sub + i, 0)),
        ] + [pl.BlockSpec((sub, r.shape[1]), lambda i: (i, 0)) for r in recvs] + extra_specs,
        out_specs=[pl.BlockSpec((sub, cols), lambda i: (i, 0)), pl.BlockSpec((8, 128), lambda i: (0, 0))],
        scratch_shapes=[
            pltpu.VMEM((nt, sub, CT), jnp.float32),
            pltpu.VMEM((nt, sub, CT), jnp.bfloat16),
            pltpu.VMEM((nt, sub, CT), jnp.bfloat16),
            pltpu.VMEM((nt, sub, CT), jnp.bfloat16),
            pltpu.VMEM((128, 128), jnp.float32),
        ],
        cost_estimate=pl.CostEstimate(
            flops=6 * rows * cols * CT, bytes_accessed=rows * cols * 12, transcendentals=rows * cols),
        compiler_params=pltpu.CompilerParams(dimension_semantics=("arbitrary",), vmem_limit_bytes=ALL_VMEM),
    )(temp, tgt, tri, own, *recvs, *extra)


def combine(stats, me):
    top = functools.reduce(jnp.maximum, [st[0:1] for _, st in stats])
    total = below = at_tgt = jnp.zeros_like(top)
    scale = jnp.exp(stats[0][1][0:1] - top)
    for index, st in stats:
        f = jnp.exp(st[0:1] - top)
        s = st[1:2] * f
        total += s
        at_tgt += st[2:3] * f
        below += jnp.where(index < me, s, 0.0)
    inv = 1.0 / total
    first = lax.broadcasted_iota(jnp.int32, (128, 128), 0) == 0
    return jnp.where(first, scale * inv, below * inv).T, at_tgt * inv


def merged(ct, at_tgt, blk, at, rows):
    row = lax.broadcasted_iota(jnp.int32, ct.shape, 0)
    lane = lax.broadcasted_iota(jnp.int32, ct.shape, 1)
    return jnp.where((row == blk) & (lane >= at) & (lane < at + rows), at_tgt, ct)


def final_kernel(pos_ref, pre_ref, st_ref, mine_ref, other_ref, ctin_ref, *refs, blk, at, rows):
    out_ref, ct_ref, ab_s = refs[-3:]
    step = pl.program_id(0)
    sub = pre_ref.shape[0]

    @pl.when(step == 0)
    def _():
        voc, hid = pos_ref[0], pos_ref[1]
        nv = mine_ref.shape[0]
        me = voc * 2 + hid
        own = st_ref[...]
        stats = [(me, own)]
        real = lax.broadcasted_iota(jnp.int32, own.shape, 0) == 0
        for v in range(nv):
            stats.append((v * 2 + hid, jnp.where(real | (v != voc), mine_ref[v], 0.0)))
            stats.append((v * 2 + 1 - hid, other_ref[v]))
        ab, at_tgt = combine(stats, me)
        ab_s[...] = ab
        ct_ref[...] = merged(ctin_ref[...], at_tgt, blk, at, rows)

    ab = ab_s[pl.ds(pl.multiple_of(at + step * sub, sub), sub), :]
    out_ref[...] = pre_ref[...] * ab[:, 0:1] + ab[:, 1:2]


def finish(pos, pre, st, mine, other, out, ct, all_rows, blk, at, row0, deps):
    rows, cols = pre.shape
    sub = min(SUB, rows)
    tail = ([] if out is None else [out]) + list(deps)
    small = pl.BlockSpec((8, 128), lambda i, s: (0, 0))
    wide = pl.BlockSpec(mine.shape, lambda i, s: (0, 0, 0))
    return pl.pallas_call(
        functools.partial(final_kernel, blk=blk, at=at, rows=rows),
        out_shape=[jax.ShapeDtypeStruct((all_rows, cols), jnp.float32), jax.ShapeDtypeStruct((8, 128), jnp.float32)],
        grid_spec=pltpu.PrefetchScalarGridSpec(
            num_scalar_prefetch=1,
            grid=(rows // sub,),
            in_specs=[pl.BlockSpec((sub, cols), lambda i, s: (i, 0)), small, wide, wide, small]
            + [pl.BlockSpec(memory_space=pl.ANY)] * len(tail),
            out_specs=[pl.BlockSpec((sub, cols), lambda i, s: (row0 // sub + i, 0)), small],
            scratch_shapes=[pltpu.VMEM((128, 128), jnp.float32)],
        ),
        input_output_aliases={} if out is None else {6: 0},
        cost_estimate=pl.CostEstimate(flops=64 * rows * cols, bytes_accessed=rows * cols * 8, transcendentals=0),
        compiler_params=pltpu.CompilerParams(dimension_semantics=("arbitrary",), vmem_limit_bytes=ALL_VMEM),
    )(pos, pre, st, mine, other, ct, *tail)


def exchange_kernel(st_ref, ab_ref, at_tgt_ref, slots, send_sem, recv_sem):
    voc = lax.axis_index("vocab")
    hid = lax.axis_index("hid")
    steps = [(dv, dh) for dv in range(4) for dh in range(2)][1:]
    barrier = pltpu.get_barrier_semaphore()
    for dv, dh in steps:
        pl.semaphore_signal(
            barrier, inc=1, device_id={"vocab": lax.rem(voc + dv, 4), "hid": lax.rem(hid + dh, 2)},
            device_id_type=pl.DeviceIdType.MESH)
    pl.semaphore_wait(barrier, len(steps))
    copies = []
    for i, (dv, dh) in enumerate(steps):
        copy = pltpu.make_async_remote_copy(
            src_ref=st_ref,
            dst_ref=slots.at[i],
            send_sem=send_sem.at[i],
            recv_sem=recv_sem.at[i],
            device_id={"vocab": lax.rem(voc + dv, 4), "hid": lax.rem(hid + dh, 2)},
            device_id_type=pl.DeviceIdType.MESH,
        )
        copy.start()
        copies.append(copy)
    for copy in copies:
        copy.wait()
    me = voc * 2 + hid
    stats = [(me, st_ref[...])]
    for i, (dv, dh) in enumerate(steps):
        stats.append((lax.rem(voc + 4 - dv, 4) * 2 + lax.rem(hid + 2 - dh, 2), slots[i]))
    ab, at_tgt = combine(stats, me)
    ab_ref[...] = ab
    at_tgt_ref[...] = jnp.broadcast_to(at_tgt, at_tgt_ref.shape)


def exchange(st):
    return pl.pallas_call(
        exchange_kernel,
        out_shape=[jax.ShapeDtypeStruct((128, 128), jnp.float32), jax.ShapeDtypeStruct((8, 128), jnp.float32)],
        in_specs=[pl.BlockSpec(memory_space=pltpu.VMEM)],
        out_specs=[pl.BlockSpec(memory_space=pltpu.VMEM)] * 2,
        scratch_shapes=[
            pltpu.VMEM((7, 8, 128), jnp.float32),
            pltpu.SemaphoreType.DMA((7,)),
            pltpu.SemaphoreType.DMA((7,)),
        ],
        compiler_params=pltpu.CompilerParams(collective_id=0, has_side_effects=True, vmem_limit_bytes=ALL_VMEM),
        name="exchange",
    )(st)


def last_kernel(ab_ref, at_tgt_ref, ctin_ref, *refs, blk, at, rows, nparts):
    out_ref, ct_ref = refs[-2:]
    step = pl.program_id(0)
    sub = out_ref.shape[0]
    ab = ab_ref[pl.ds(pl.multiple_of(at + step * sub, sub), sub), :]
    ct_ref[...] = merged(ctin_ref[...], at_tgt_ref[...], blk, at, rows)
    for i in range(nparts):
        @pl.when(step == i)
        def _(pre_ref=refs[i]):
            out_ref[...] = pre_ref[...] * ab[:, 0:1] + ab[:, 1:2]


def finish_last(ab, at_tgt, ct, pres, out, blk, at, row0, deps):
    sub, cols = pres[0].shape
    n = len(pres)
    small = pl.BlockSpec((8, 128), lambda i: (0, 0))
    return pl.pallas_call(
        functools.partial(last_kernel, blk=blk, at=at, rows=sub * n, nparts=n),
        grid=(n,),
        out_shape=[jax.ShapeDtypeStruct(out.shape, jnp.float32), jax.ShapeDtypeStruct((8, 128), jnp.float32)],
        in_specs=[pl.BlockSpec((128, 128), lambda i: (0, 0)), small, small]
        + [pl.BlockSpec((sub, cols), lambda i: (0, 0))] * n
        + [pl.BlockSpec(memory_space=pl.ANY)] * (1 + len(deps)),
        out_specs=[pl.BlockSpec((sub, cols), lambda i: (row0 // sub + i, 0)), small],
        input_output_aliases={3 + n: 0},
        compiler_params=pltpu.CompilerParams(dimension_semantics=("arbitrary",), vmem_limit_bytes=ALL_VMEM),
        name="finish_last",
    )(ab, at_tgt, ct, *pres, out, *deps)


def solution(mesh):
    def pipeline(h, w, temp, tgt):
        rows_all = h.shape[0]
        cols = w.shape[1] // 2
        hid = lax.axis_index("hid")
        voc = lax.axis_index("vocab")
        own_half = hid.astype(jnp.int32).reshape(1)
        peer_half = (1 - hid).astype(jnp.int32).reshape(1)
        pos = jnp.stack([voc, hid]).astype(jnp.int32)
        temp2 = temp[:, None]
        tgt2 = (tgt - (voc * 2 + hid) * cols)[:, None]
        tri = (lax.broadcasted_iota(jnp.int32, (CT, CT), 0) <= lax.broadcasted_iota(jnp.int32, (CT, CT), 1)).astype(jnp.bfloat16)
        swap = [(0, 1), (1, 0)]

        blk = 128
        nblk = rows_all // blk
        last = (64, 32, 16, 16)
        tn = 7 * CT
        ht = cols // tn

        units = [(b, 0, blk) for b in range(nblk - 1)]
        units += [(nblk - 1, sum(last[:i]), r) for i, r in enumerate(last)]
        nu = len(units)
        parts = {}
        owns = {}
        tok = None

        def peer(b):
            nonlocal tok
            if b >= nblk:
                return
            splits = last if b == nblk - 1 else (blk,)
            outs = partial_products(h, w, peer_half, b * blk, splits, 0, ht, tn, ht, (tok,))
            tok = outs[0]
            for i, o in enumerate(outs):
                parts[b + i] = [o]

        def mine_half(b):
            nonlocal tok
            if b >= nblk:
                return
            tok = owns[b] = partial_products(h, w, own_half, b * blk, (blk,), 0, ht, tn, ht, (tok,))[0]

        tok = partial_products(h, w, peer_half, 0, (blk,), 0, 2, tn // 2, 2 * ht)[0]
        parts[0] = [tok]
        tok = partial_products(h, w, peer_half, 0, (blk,), 1, ht - 1, tn, ht, (tok,))[0]
        parts[0].append(tok)
        peer(1)
        peer(2)
        mine_half(0)
        mine_half(1)

        def send(arrays):
            return [lax.ppermute(a, "hid", swap) for a in arrays]

        recvs = {0: send(parts[0][:1]) + send(parts[0][1:]), 1: send(parts[1])}
        pres, stats = {}, {}
        out = None
        ct = jnp.zeros((nblk, blk), jnp.float32)

        def close(k):
            nonlocal out, ct, tok
            b, at, _ = units[k]
            out, ct = finish(pos, pres[k], *stats[k], out, ct, rows_all, b, at, b * blk + at, (tok,))
            tok = ct

        prev = None
        for k, (b, at, rows) in enumerate(units):
            pres[k], st = local_prefix(
                temp2, tgt2, tri, owns[b], at, recvs[k], rows, b * blk + at, prev, (tok,))
            tok = st
            if k == nu - 2:
                prev = st
                close(k - 1)
                continue
            if k == nu - 1:
                ab, at_tgt = exchange(st)
                at = units[k - 1][1]
                out, ct = finish_last(ab, at_tgt, ct, [pres[k - 1], pres[k]], out, b, at, b * blk + at, (tok,))
                break
            mine = lax.all_gather(st, "vocab")
            if k + 2 < nu:
                *sent, mine = lax.optimization_barrier((*parts[k + 2], mine))
                stats[k] = (st, mine, send([mine])[0])
                recvs[k + 2] = send(sent)
            tok = mine
            if k >= 1:
                close(k - 1)
            peer(k + 3)
            mine_half(k + 2)
        return out, ct.reshape(rows_all)

    return jax.shard_map(
        pipeline,
        mesh=mesh,
        in_specs=(P("data", "hid"), P("hid", "vocab"), P("data"), P("data")),
        out_specs=(P("data", ("vocab", "hid")), P("data")),
        check_vma=False,
    )
```

```python
import functools

import jax
import jax.numpy as jnp
from jax import lax
from jax.experimental import pallas as pl
from jax.experimental.pallas import tpu as pltpu
from jax.sharding import PartitionSpec as P


CT = 256
SUB = 32
ALL_VMEM = 67043328


def mm_kernel(sel_ref, h_ref, w_ref, *refs, splits):
    out_refs = refs[len(refs) - len(splits):]
    res = jnp.dot(h_ref[...], w_ref[...], preferred_element_type=jnp.float32)
    at = 0
    for ref, rows in zip(out_refs, splits):
        ref[...] = res[at:at + rows]
        at += rows


def partial_products(h, w, half, row0, splits, tile0, ntiles, tn, half_tiles, deps=()):
    rows = sum(splits)
    depth = h.shape[1]
    cols = ntiles * tn
    return pl.pallas_call(
        functools.partial(mm_kernel, splits=splits),
        out_shape=[jax.ShapeDtypeStruct((r, cols), jnp.float32) for r in splits],
        grid_spec=pltpu.PrefetchScalarGridSpec(
            num_scalar_prefetch=1,
            grid=(ntiles,),
            in_specs=[
                pl.BlockSpec((rows, depth), lambda j, s: (row0 // rows, 0)),
                pl.BlockSpec((depth, tn), lambda j, s: (0, s[0] * half_tiles + tile0 + j)),
            ] + [pl.BlockSpec(memory_space=pl.ANY)] * len(deps),
            out_specs=[pl.BlockSpec((r, tn), lambda j, s: (0, j)) for r in splits],
        ),
        cost_estimate=pl.CostEstimate(
            flops=2 * rows * depth * cols, bytes_accessed=depth * cols * 2 + rows * cols * 4, transcendentals=0),
        compiler_params=pltpu.CompilerParams(dimension_semantics=("arbitrary",), vmem_limit_bytes=ALL_VMEM),
    )(half, h, w, *deps)


def local_kernel(temp_ref, tgt_ref, tri_ref, own_ref, *refs, npieces, has_prev, skip, at, group, share):
    recv_refs = refs[:npieces]
    prev_ref = refs[npieces] if has_prev else None
    if share:
        pre_ref, ab_ref, at_tgt_ref, z_s, hi_s, mid_s, lo_s, st_s, st_ref, slots, send_sem, recv_sem = refs[npieces + has_prev + skip:]
        announce()
    else:
        pre_ref, st_ref, z_s, hi_s, mid_s, lo_s, st_s = refs[npieces + has_prev + skip:]
    step, nsteps = pl.program_id(0), pl.num_programs(0)
    rows = own_ref.shape[0]
    nt = own_ref.shape[1] // CT
    temp = jnp.broadcast_to(temp_ref[...], (rows, CT))
    mx = jnp.full((rows, CT), -jnp.inf, jnp.float32)

    def add_tile(t, part, mx):
        z = (own_ref[:, pl.ds(pl.multiple_of(t * CT, CT), CT)] + part) * temp
        z_s[t] = z
        return jnp.maximum(mx, z)

    t0 = off = 0
    for i, ref in enumerate(recv_refs):
        n, rest = divmod(ref.shape[1] - off, CT)

        def max_step(j, mx, ref=ref, t0=t0, off=off):
            return add_tile(t0 + j, ref[:, pl.ds(pl.multiple_of(off + j * CT, 128), CT)], mx)

        mx = lax.fori_loop(0, n, max_step, mx, unroll=max(u for u in range(1, 8) if n % u == 0))
        t0, off = t0 + n, 0
        if rest:
            off = CT - rest
            both = jnp.concatenate([ref[:, ref.shape[1] - rest:], recv_refs[i + 1][:, :off]], axis=1)
            mx = add_tile(t0, both, mx)
            t0 += 1
    m = jnp.max(mx, axis=1, keepdims=True)
    mb = jnp.broadcast_to(m, (rows, CT))
    tgt = jnp.broadcast_to(tgt_ref[...], (rows, CT))
    col = lax.broadcasted_iota(jnp.int32, (rows, CT), 1)
    rel = tgt - col

    def exp_step(j, carry):
        sacc, cacc = carry
        e = jnp.exp(z_s[j] - mb)
        hi = e.astype(jnp.bfloat16)
        r1 = e - hi.astype(jnp.float32)
        mid = r1.astype(jnp.bfloat16)
        lo = (r1 - mid.astype(jnp.float32)).astype(jnp.bfloat16)
        hi_s[j] = hi
        mid_s[j] = mid
        lo_s[j] = lo
        return sacc + e, cacc + jnp.where(rel >= j * CT, e, 0.0)

    zero = jnp.zeros((rows, CT), jnp.float32)
    sacc, cacc = lax.fori_loop(0, nt, exp_step, (zero, zero), unroll=7)
    s = jnp.sum(sacc, axis=1, keepdims=True)
    c = jnp.sum(cacc, axis=1, keepdims=True)
    lane = lax.broadcasted_iota(jnp.int32, (rows, 128), 1)

    @pl.when(step == 0)
    def _():
        st_s[...] = jnp.zeros_like(st_s)

    st_s[pl.ds(pl.multiple_of(at + step * rows, rows), rows), :] = jnp.where(
        lane == 0, m, jnp.where(lane == 1, s, jnp.where(lane == 2, c, 0.0)))

    @pl.when(step == nsteps - 1)
    def _():
        st = st_s[...].T[0:8]
        st_ref[...] = st + prev_ref[...] if has_prev else st

    if share:
        copies = spread(st_ref, slots, send_sem, recv_sem)
    tri = tri_ref[...]

    def prefix_step(g, carry):
        span = pl.ds(g * group, group)
        pre = jnp.dot(hi_s[span].reshape(group * rows, CT), tri, preferred_element_type=jnp.float32)
        pre += jnp.dot(mid_s[span].reshape(group * rows, CT), tri, preferred_element_type=jnp.float32)
        pre += jnp.dot(lo_s[span].reshape(group * rows, CT), tri, preferred_element_type=jnp.float32)
        for k in range(group):
            blk = pre[k * rows:(k + 1) * rows]
            dst = pl.ds(pl.multiple_of((g * group + k) * CT, CT), CT)
            pre_ref[:, dst] = blk + carry
            carry = carry + jnp.broadcast_to(blk[:, CT - 1:CT], (rows, CT))
        return carry

    lax.fori_loop(0, nt // group, prefix_step, zero)
    if share:
        gather(copies, st_ref, slots, ab_ref, at_tgt_ref)


def local_prefix(temp, tgt, tri, own, at, recvs, rows, row0, prev, deps, share=False):
    cols = own.shape[1]
    nt = cols // CT
    sub = min(SUB, rows)
    small = (128, 8) if share else (8,)
    extra = ([] if prev is None else [prev]) + list(deps)
    extra_specs = ([] if prev is None else [pl.BlockSpec((8, 128), lambda i: (0, 0))])
    extra_specs += [pl.BlockSpec(memory_space=pl.ANY)] * len(deps)
    return pl.pallas_call(
        functools.partial(
            local_kernel, npieces=len(recvs), has_prev=int(prev is not None), skip=len(deps), at=at, group=7, share=share),
        grid=(rows // sub,),
        out_shape=[jax.ShapeDtypeStruct((rows, cols), jnp.float32)]
        + [jax.ShapeDtypeStruct((n, 128), jnp.float32) for n in small],
        in_specs=[
            pl.BlockSpec((sub, 1), lambda i: (row0 // sub + i, 0)),
            pl.BlockSpec((sub, 1), lambda i: (row0 // sub + i, 0)),
            pl.BlockSpec((CT, CT), lambda i: (0, 0)),
            pl.BlockSpec((sub, cols), lambda i: (at // sub + i, 0)),
        ] + [pl.BlockSpec((sub, r.shape[1]), lambda i: (i, 0)) for r in recvs] + extra_specs,
        out_specs=[pl.BlockSpec((sub, cols), lambda i: (i, 0))]
        + [pl.BlockSpec((n, 128), lambda i: (0, 0)) for n in small],
        scratch_shapes=[
            pltpu.VMEM((nt, sub, CT), jnp.float32),
            pltpu.VMEM((nt, sub, CT), jnp.bfloat16),
            pltpu.VMEM((nt, sub, CT), jnp.bfloat16),
            pltpu.VMEM((nt, sub, CT), jnp.bfloat16),
            pltpu.VMEM((128, 128), jnp.float32),
        ] + ([
            pltpu.VMEM((8, 128), jnp.float32),
            pltpu.VMEM((7, 8, 128), jnp.float32),
            pltpu.SemaphoreType.DMA((7,)),
            pltpu.SemaphoreType.DMA((7,)),
        ] if share else []),
        cost_estimate=pl.CostEstimate(
            flops=6 * rows * cols * CT, bytes_accessed=rows * cols * 12, transcendentals=rows * cols),
        compiler_params=pltpu.CompilerParams(
            dimension_semantics=("arbitrary",), vmem_limit_bytes=ALL_VMEM,
            **(dict(collective_id=0, has_side_effects=True) if share else {})),
    )(temp, tgt, tri, own, *recvs, *extra)


STEPS = [(dv, dh) for dv in range(4) for dh in range(2)][1:]


def device(dv, dh):
    return {"vocab": lax.rem(lax.axis_index("vocab") + dv, 4), "hid": lax.rem(lax.axis_index("hid") + dh, 2)}


def announce():
    barrier = pltpu.get_barrier_semaphore()
    for dv, dh in STEPS:
        pl.semaphore_signal(barrier, inc=1, device_id=device(dv, dh), device_id_type=pl.DeviceIdType.MESH)


def spread(st_ref, slots, send_sem, recv_sem):
    pl.semaphore_wait(pltpu.get_barrier_semaphore(), len(STEPS))
    copies = []
    for i, (dv, dh) in enumerate(STEPS):
        copy = pltpu.make_async_remote_copy(
            src_ref=st_ref,
            dst_ref=slots.at[i],
            send_sem=send_sem.at[i],
            recv_sem=recv_sem.at[i],
            device_id=device(dv, dh),
            device_id_type=pl.DeviceIdType.MESH,
        )
        copy.start()
        copies.append(copy)
    return copies


def gather(copies, st_ref, slots, ab_ref, at_tgt_ref):
    for copy in copies:
        copy.wait()
    voc = lax.axis_index("vocab")
    hid = lax.axis_index("hid")
    me = voc * 2 + hid
    stats = []
    for i, (dv, dh) in enumerate(STEPS):
        index = lax.rem(voc + 4 - dv, 4) * 2 + lax.rem(hid + 2 - dh, 2)
        st = slots[i]
        stats.append((st, jnp.where(index < me, st[1:2], 0.0)))
    ab, at_tgt = combine(st_ref[...], stats)
    ab_ref[...] = ab
    at_tgt_ref[...] = jnp.broadcast_to(at_tgt, at_tgt_ref.shape)


def combine(own, others):
    top = functools.reduce(jnp.maximum, [st[0:1] for st, _ in others], own[0:1])
    scale = jnp.exp(own[0:1] - top)
    total = own[1:2] * scale
    at_tgt = own[2:3] * scale
    below = jnp.zeros_like(top)
    for st, lower in others:
        f = jnp.exp(st[0:1] - top)
        total += st[1:2] * f
        at_tgt += st[2:3] * f
        below += lower * f
    inv = 1.0 / total
    first = lax.broadcasted_iota(jnp.int32, (128, 128), 0) == 0
    return jnp.where(first, scale * inv, below * inv).T, at_tgt * inv


def group_kernel(pos_ref, mine_ref, group_ref):
    voc, hid = pos_ref[0], pos_ref[1]
    nv = mine_ref.shape[0]
    top = functools.reduce(jnp.maximum, [mine_ref[v, 0:1] for v in range(nv)])
    total = at_tgt = below = jnp.zeros_like(top)
    for v in range(nv):
        f = jnp.exp(mine_ref[v, 0:1] - top)
        s = mine_ref[v, 1:2] * f
        total += s
        at_tgt += mine_ref[v, 2:3] * f
        below += jnp.where((v < voc) | ((v == voc) & (hid == 0)), s, 0.0)
    row = lax.broadcasted_iota(jnp.int32, group_ref.shape, 0)
    group_ref[...] = jnp.where(row == 0, top, jnp.where(row == 1, total, jnp.where(row == 2, at_tgt, below)))


def group_stats(pos, mine):
    return pl.pallas_call(
        group_kernel,
        out_shape=jax.ShapeDtypeStruct(mine.shape[1:], jnp.float32),
        grid_spec=pltpu.PrefetchScalarGridSpec(
            num_scalar_prefetch=1,
            grid=(1,),
            in_specs=[pl.BlockSpec(mine.shape, lambda i, s: (0, 0, 0))],
            out_specs=pl.BlockSpec(mine.shape[1:], lambda i, s: (0, 0)),
        ),
        compiler_params=pltpu.CompilerParams(dimension_semantics=("arbitrary",), vmem_limit_bytes=ALL_VMEM),
        name="group_stats",
    )(pos, mine)


def merged(ct, at_tgt, blk, at, rows):
    row = lax.broadcasted_iota(jnp.int32, ct.shape, 0)
    lane = lax.broadcasted_iota(jnp.int32, ct.shape, 1)
    return jnp.where((row == blk) & (lane >= at) & (lane < at + rows), at_tgt, ct)


def final_kernel(pos_ref, pre_ref, st_ref, mine_ref, other_ref, ctin_ref, *refs, blk, at, rows):
    out_ref, ct_ref, ab_s = refs[-3:]
    step = pl.program_id(0)
    sub = pre_ref.shape[0]

    @pl.when(step == 0)
    def _():
        voc = pos_ref[0]
        own = st_ref[...]
        others = []
        row = lax.broadcasted_iota(jnp.int32, own.shape, 0)
        for v in range(mine_ref.shape[0]):
            st = jnp.where((row == 0) | (v != voc), mine_ref[v], 0.0)
            others.append((st, jnp.where(v < voc, st[1:2], 0.0)))
        others.append((other_ref[...], other_ref[3:4]))
        ab, at_tgt = combine(own, others)
        ab_s[...] = ab
        ct_ref[...] = merged(ctin_ref[...], at_tgt, blk, at, rows)

    ab = ab_s[pl.ds(pl.multiple_of(at + step * sub, sub), sub), :]
    out_ref[...] = pre_ref[...] * ab[:, 0:1] + ab[:, 1:2]


def finish(pos, pre, st, mine, other, out, ct, all_rows, blk, at, row0, deps):
    rows, cols = pre.shape
    sub = min(SUB, rows)
    tail = ([] if out is None else [out]) + list(deps)
    small = pl.BlockSpec((8, 128), lambda i, s: (0, 0))
    wide = pl.BlockSpec(mine.shape, lambda i, s: (0, 0, 0))
    return pl.pallas_call(
        functools.partial(final_kernel, blk=blk, at=at, rows=rows),
        out_shape=[jax.ShapeDtypeStruct((all_rows, cols), jnp.float32), jax.ShapeDtypeStruct((8, 128), jnp.float32)],
        grid_spec=pltpu.PrefetchScalarGridSpec(
            num_scalar_prefetch=1,
            grid=(rows // sub,),
            in_specs=[pl.BlockSpec((sub, cols), lambda i, s: (i, 0)), small, wide, small, small]
            + [pl.BlockSpec(memory_space=pl.ANY)] * len(tail),
            out_specs=[pl.BlockSpec((sub, cols), lambda i, s: (row0 // sub + i, 0)), small],
            scratch_shapes=[pltpu.VMEM((128, 128), jnp.float32)],
        ),
        input_output_aliases={} if out is None else {6: 0},
        cost_estimate=pl.CostEstimate(flops=64 * rows * cols, bytes_accessed=rows * cols * 8, transcendentals=0),
        compiler_params=pltpu.CompilerParams(dimension_semantics=("arbitrary",), vmem_limit_bytes=ALL_VMEM),
    )(pos, pre, st, mine, other, ct, *tail)


def last_kernel(ab_ref, at_tgt_ref, ctin_ref, *refs, blk, at, rows, nparts):
    out_ref, ct_ref = refs[-2:]
    step = pl.program_id(0)
    sub = out_ref.shape[0]
    ab = ab_ref[pl.ds(pl.multiple_of(at + step * sub, sub), sub), :]
    ct_ref[...] = merged(ctin_ref[...], at_tgt_ref[...], blk, at, rows)
    for i in range(nparts):
        @pl.when(step == i)
        def _(pre_ref=refs[i]):
            out_ref[...] = pre_ref[...] * ab[:, 0:1] + ab[:, 1:2]


def finish_last(ab, at_tgt, ct, pres, out, blk, at, row0, deps):
    sub, cols = pres[0].shape
    n = len(pres)
    small = pl.BlockSpec((8, 128), lambda i: (0, 0))
    return pl.pallas_call(
        functools.partial(last_kernel, blk=blk, at=at, rows=sub * n, nparts=n),
        grid=(n,),
        out_shape=[jax.ShapeDtypeStruct(out.shape, jnp.float32), jax.ShapeDtypeStruct((8, 128), jnp.float32)],
        in_specs=[pl.BlockSpec((128, 128), lambda i: (0, 0)), small, small]
        + [pl.BlockSpec((sub, cols), lambda i: (0, 0))] * n
        + [pl.BlockSpec(memory_space=pl.ANY)] * (1 + len(deps)),
        out_specs=[pl.BlockSpec((sub, cols), lambda i: (row0 // sub + i, 0)), small],
        input_output_aliases={3 + n: 0},
        compiler_params=pltpu.CompilerParams(dimension_semantics=("arbitrary",), vmem_limit_bytes=ALL_VMEM),
        name="finish_last",
    )(ab, at_tgt, ct, *pres, out, *deps)


def solution(mesh):
    def pipeline(h, w, temp, tgt):
        rows_all = h.shape[0]
        cols = w.shape[1] // 2
        hid = lax.axis_index("hid")
        voc = lax.axis_index("vocab")
        own_half = hid.astype(jnp.int32).reshape(1)
        peer_half = (1 - hid).astype(jnp.int32).reshape(1)
        pos = jnp.stack([voc, hid]).astype(jnp.int32)
        temp2 = temp[:, None]
        tgt2 = (tgt - (voc * 2 + hid) * cols)[:, None]
        tri = (lax.broadcasted_iota(jnp.int32, (CT, CT), 0) <= lax.broadcasted_iota(jnp.int32, (CT, CT), 1)).astype(jnp.bfloat16)
        swap = [(0, 1), (1, 0)]

        blk = 128
        nblk = rows_all // blk
        last = (64, 32, 16, 16)
        tn = 7 * CT
        ht = cols // tn

        units = [(b, 0, blk) for b in range(nblk - 1)]
        units += [(nblk - 1, sum(last[:i]), r) for i, r in enumerate(last)]
        nu = len(units)
        parts = {}
        owns = {}
        tok = None

        def peer(b):
            nonlocal tok
            if b >= nblk:
                return
            splits = last if b == nblk - 1 else (blk,)
            outs = partial_products(h, w, peer_half, b * blk, splits, 0, ht, tn, ht, (tok,))
            tok = outs[0]
            for i, o in enumerate(outs):
                parts[b + i] = [o]

        def mine_half(b):
            nonlocal tok
            if b >= nblk:
                return
            tok = owns[b] = partial_products(h, w, own_half, b * blk, (blk,), 0, ht, tn, ht, (tok,))[0]

        at = 0
        parts[0] = []
        for i, n in enumerate((1, 2, 2 * ht - 3)):
            tok = partial_products(
                h, w, peer_half, 0, (blk,), at, n, tn // 2, 2 * ht, () if i == 0 else (tok,))[0]
            parts[0].append(tok)
            at += n
        peer(1)
        peer(2)
        mine_half(0)
        mine_half(1)

        def send(arrays):
            return [lax.ppermute(a, "hid", swap) for a in arrays]

        recvs = {0: [send([p])[0] for p in parts[0]], 1: send(parts[1])}
        pres, stats = {}, {}
        out = None
        ct = jnp.zeros((nblk, blk), jnp.float32)

        def close(k):
            nonlocal out, ct, tok
            b, at, _ = units[k]
            out, ct = finish(pos, pres[k], *stats[k], out, ct, rows_all, b, at, b * blk + at, (tok,))
            tok = ct

        prev = None
        for k, (b, at, rows) in enumerate(units):
            share = k == nu - 1
            pres[k], *small = local_prefix(
                temp2, tgt2, tri, owns[b], at, recvs[k], rows, b * blk + at, prev, (tok,), share)
            if share:
                at = units[k - 1][1]
                out, ct = finish_last(*small, ct, [pres[k - 1], pres[k]], out, b, at, b * blk + at, (tok,))
                break
            tok = st = small[0]
            if k == nu - 2:
                prev = st
                close(k - 1)
                continue
            mine = lax.all_gather(st, "vocab")
            grp = group_stats(pos, mine)
            *sent, grp = lax.optimization_barrier((*parts[k + 2], grp))
            stats[k] = (st, mine, send([grp])[0])
            recvs[k + 2] = send(sent)
            tok = grp
            if k >= 1:
                close(k - 1)
            peer(k + 3)
            mine_half(k + 2)
        return out, ct.reshape(rows_all)

    return jax.shard_map(
        pipeline,
        mesh=mesh,
        in_specs=(P("data", "hid"), P("hid", "vocab"), P("data"), P("data")),
        out_specs=(P("data", ("vocab", "hid")), P("data")),
        check_vma=False,
    )
```

```python
import functools
import math

import jax
import jax.numpy as jnp
from jax import lax
from jax.experimental import pallas as pl
from jax.experimental.pallas import tpu as pltpu
from jax.sharding import PartitionSpec as P


CT = 256
SUB = 32
ALL_VMEM = 67043328


def mm_kernel(sel_ref, h_ref, w_ref, *refs, splits, ksteps):
    out_refs = refs[len(refs) - len(splits):]
    res = jnp.dot(h_ref[...], w_ref[...], preferred_element_type=jnp.float32)

    def put(add):
        at = 0
        for ref, rows in zip(out_refs, splits):
            ref[...] = ref[...] + res[at:at + rows] if add else res[at:at + rows]
            at += rows

    if ksteps == 1:
        put(False)
    else:
        pl.when(pl.program_id(1) == 0)(functools.partial(put, False))
        pl.when(pl.program_id(1) > 0)(functools.partial(put, True))


def partial_products(h, w, half, row0, splits, tile0, ntiles, tn, half_tiles, deps=(), ksteps=1):
    rows = sum(splits)
    depth = h.shape[1]
    cols = ntiles * tn
    return pl.pallas_call(
        functools.partial(mm_kernel, splits=splits, ksteps=ksteps),
        out_shape=[jax.ShapeDtypeStruct((r, cols), jnp.float32) for r in splits],
        grid_spec=pltpu.PrefetchScalarGridSpec(
            num_scalar_prefetch=1,
            grid=(ntiles, ksteps),
            in_specs=[
                pl.BlockSpec((rows, depth // ksteps), lambda j, k, s: (row0 // rows, k)),
                pl.BlockSpec((depth // ksteps, tn), lambda j, k, s: (k, s[0] * half_tiles + tile0 + j)),
            ] + [pl.BlockSpec(memory_space=pl.ANY)] * len(deps),
            out_specs=[pl.BlockSpec((r, tn), lambda j, k, s: (0, j)) for r in splits],
        ),
        cost_estimate=pl.CostEstimate(
            flops=2 * rows * depth * cols, bytes_accessed=depth * cols * 2 + rows * cols * 4, transcendentals=0),
        compiler_params=pltpu.CompilerParams(dimension_semantics=("arbitrary", "arbitrary"), vmem_limit_bytes=ALL_VMEM),
    )(half, h, w, *deps)


def local_kernel(temp_ref, tgt_ref, tri_ref, own_ref, *refs, npieces, has_prev, skip, at, group, share):
    recv_refs = refs[:npieces]
    prev_ref = refs[npieces] if has_prev else None
    if share:
        pre_ref, ab_ref, at_tgt_ref, z_s, hi_s, mid_s, lo_s, st_s, st_ref, slots, send_sem, recv_sem, pre_s, out_sem = refs[npieces + has_prev + skip:]
        announce()
        pre_hbm, pre_ref = pre_ref, pre_s
    else:
        pre_ref, st_ref, z_s, hi_s, mid_s, lo_s, st_s = refs[npieces + has_prev + skip:]
    step, nsteps = pl.program_id(0), pl.num_programs(0)
    rows = own_ref.shape[0]
    nt = own_ref.shape[1] // CT
    temp = jnp.broadcast_to(temp_ref[...], (rows, CT))
    mx = jnp.full((rows, CT), -jnp.inf, jnp.float32)

    def add_tile(t, part, mx):
        z = (own_ref[:, pl.ds(pl.multiple_of(t * CT, CT), CT)] + part) * temp
        z_s[t] = z
        return jnp.maximum(mx, z)

    t0 = off = 0
    for i, ref in enumerate(recv_refs):
        n, rest = divmod(ref.shape[1] - off, CT)

        def max_step(j, mx, ref=ref, t0=t0, off=off):
            return add_tile(t0 + j, ref[:, pl.ds(pl.multiple_of(off + j * CT, 128), CT)], mx)

        mx = lax.fori_loop(0, n, max_step, mx, unroll=max(u for u in range(1, 8) if n % u == 0))
        t0, off = t0 + n, 0
        if rest:
            off = CT - rest
            both = jnp.concatenate([ref[:, ref.shape[1] - rest:], recv_refs[i + 1][:, :off]], axis=1)
            mx = add_tile(t0, both, mx)
            t0 += 1
    m = jnp.max(mx, axis=1, keepdims=True)
    mb = jnp.broadcast_to(m, (rows, CT))
    tgt = jnp.broadcast_to(tgt_ref[...], (rows, CT))
    col = lax.broadcasted_iota(jnp.int32, (rows, CT), 1)
    rel = tgt - col

    def exp_step(j, carry):
        sacc, cacc = carry
        e = jnp.exp(z_s[j] - mb)
        hi = e.astype(jnp.bfloat16)
        r1 = e - hi.astype(jnp.float32)
        mid = r1.astype(jnp.bfloat16)
        lo = (r1 - mid.astype(jnp.float32)).astype(jnp.bfloat16)
        hi_s[j] = hi
        mid_s[j] = mid
        lo_s[j] = lo
        return sacc + e, cacc + jnp.where(rel >= j * CT, e, 0.0)

    zero = jnp.zeros((rows, CT), jnp.float32)
    sacc, cacc = lax.fori_loop(0, nt, exp_step, (zero, zero), unroll=7)
    s = jnp.sum(sacc, axis=1, keepdims=True)
    c = jnp.sum(cacc, axis=1, keepdims=True)
    lane = lax.broadcasted_iota(jnp.int32, (rows, 128), 1)

    @pl.when(step == 0)
    def _():
        st_s[...] = jnp.zeros_like(st_s)

    st_s[pl.ds(pl.multiple_of(at + step * rows, rows), rows), :] = jnp.where(
        lane == 0, m, jnp.where(lane == 1, s, jnp.where(lane == 2, c, 0.0)))

    @pl.when(step == nsteps - 1)
    def _():
        st = st_s[...].T[0:8]
        st_ref[...] = st + prev_ref[...] if has_prev else st

    if share:
        copies = spread(st_ref, slots, send_sem, recv_sem)
    tri = tri_ref[...]

    def prefix_step(g, carry):
        span = pl.ds(g * group, group)
        pre = jnp.dot(hi_s[span].reshape(group * rows, CT), tri, preferred_element_type=jnp.float32)
        pre += jnp.dot(mid_s[span].reshape(group * rows, CT), tri, preferred_element_type=jnp.float32)
        pre += jnp.dot(lo_s[span].reshape(group * rows, CT), tri, preferred_element_type=jnp.float32)
        for k in range(group):
            blk = pre[k * rows:(k + 1) * rows]
            dst = pl.ds(pl.multiple_of((g * group + k) * CT, CT), CT)
            pre_ref[:, dst] = blk + carry
            carry = carry + jnp.broadcast_to(blk[:, CT - 1:CT], (rows, CT))
        return carry

    lax.fori_loop(0, nt // group, prefix_step, zero)
    if share:
        put = pltpu.make_async_copy(pre_ref, pre_hbm, out_sem)
        put.start()
        gather(copies, st_ref, slots, ab_ref, at_tgt_ref)
        put.wait()


def local_prefix(temp, tgt, tri, own, at, recvs, rows, row0, prev, deps, share=False):
    cols = own.shape[1]
    nt = cols // CT
    sub = math.gcd(SUB, rows, at)
    small = (128, 8) if share else (8,)
    extra = ([] if prev is None else [prev]) + list(deps)
    extra_specs = ([] if prev is None else [pl.BlockSpec((8, 128), lambda i: (0, 0))])
    extra_specs += [pl.BlockSpec(memory_space=pl.ANY)] * len(deps)
    return pl.pallas_call(
        functools.partial(
            local_kernel, npieces=len(recvs), has_prev=int(prev is not None), skip=len(deps), at=at, group=7, share=share),
        grid=(rows // sub,),
        out_shape=[jax.ShapeDtypeStruct((rows, cols), jnp.float32)]
        + [jax.ShapeDtypeStruct((n, 128), jnp.float32) for n in small],
        in_specs=[
            pl.BlockSpec((sub, 1), lambda i: (row0 // sub + i, 0)),
            pl.BlockSpec((sub, 1), lambda i: (row0 // sub + i, 0)),
            pl.BlockSpec((CT, CT), lambda i: (0, 0)),
            pl.BlockSpec((sub, cols), lambda i: (at // sub + i, 0)),
        ] + [pl.BlockSpec((sub, r.shape[1]), lambda i: (i, 0)) for r in recvs] + extra_specs,
        out_specs=[pl.BlockSpec(memory_space=pl.ANY) if share else pl.BlockSpec((sub, cols), lambda i: (i, 0))]
        + [pl.BlockSpec((n, 128), lambda i: (0, 0)) for n in small],
        scratch_shapes=[
            pltpu.VMEM((nt, sub, CT), jnp.float32),
            pltpu.VMEM((nt, sub, CT), jnp.bfloat16),
            pltpu.VMEM((nt, sub, CT), jnp.bfloat16),
            pltpu.VMEM((nt, sub, CT), jnp.bfloat16),
            pltpu.VMEM((128, 128), jnp.float32),
        ] + ([
            pltpu.VMEM((8, 128), jnp.float32),
            pltpu.VMEM((7, 8, 128), jnp.float32),
            pltpu.SemaphoreType.DMA((7,)),
            pltpu.SemaphoreType.DMA((7,)),
            pltpu.VMEM((rows, cols), jnp.float32),
            pltpu.SemaphoreType.DMA,
        ] if share else []),
        cost_estimate=pl.CostEstimate(
            flops=6 * rows * cols * CT, bytes_accessed=rows * cols * 12, transcendentals=rows * cols),
        compiler_params=pltpu.CompilerParams(
            dimension_semantics=("arbitrary",), vmem_limit_bytes=ALL_VMEM,
            **(dict(collective_id=0, has_side_effects=True) if share else {})),
    )(temp, tgt, tri, own, *recvs, *extra)


STEPS = [(dv, dh) for dv in range(4) for dh in range(2)][1:]


def device(dv, dh):
    return {"vocab": lax.rem(lax.axis_index("vocab") + dv, 4), "hid": lax.rem(lax.axis_index("hid") + dh, 2)}


def announce():
    barrier = pltpu.get_barrier_semaphore()
    for dv, dh in STEPS:
        pl.semaphore_signal(barrier, inc=1, device_id=device(dv, dh), device_id_type=pl.DeviceIdType.MESH)


def spread(st_ref, slots, send_sem, recv_sem):
    pl.semaphore_wait(pltpu.get_barrier_semaphore(), len(STEPS))
    copies = []
    for i, (dv, dh) in enumerate(STEPS):
        copy = pltpu.make_async_remote_copy(
            src_ref=st_ref,
            dst_ref=slots.at[i],
            send_sem=send_sem.at[i],
            recv_sem=recv_sem.at[i],
            device_id=device(dv, dh),
            device_id_type=pl.DeviceIdType.MESH,
        )
        copy.start()
        copies.append(copy)
    return copies


def gather(copies, st_ref, slots, ab_ref, at_tgt_ref):
    for copy in copies:
        copy.wait()
    voc = lax.axis_index("vocab")
    hid = lax.axis_index("hid")
    me = voc * 2 + hid
    stats = []
    for i, (dv, dh) in enumerate(STEPS):
        index = lax.rem(voc + 4 - dv, 4) * 2 + lax.rem(hid + 2 - dh, 2)
        st = slots[i]
        stats.append((st, jnp.where(index < me, st[1:2], 0.0)))
    ab, at_tgt = combine(st_ref[...], stats)
    ab_ref[...] = ab
    at_tgt_ref[...] = jnp.broadcast_to(at_tgt, at_tgt_ref.shape)


def combine(own, others):
    top = functools.reduce(jnp.maximum, [st[0:1] for st, _ in others], own[0:1])
    scale = jnp.exp(own[0:1] - top)
    total = own[1:2] * scale
    at_tgt = own[2:3] * scale
    below = jnp.zeros_like(top)
    for st, lower in others:
        f = jnp.exp(st[0:1] - top)
        total += st[1:2] * f
        at_tgt += st[2:3] * f
        below += lower * f
    inv = 1.0 / total
    first = lax.broadcasted_iota(jnp.int32, (128, 128), 0) == 0
    return jnp.where(first, scale * inv, below * inv).T, at_tgt * inv


def group_kernel(pos_ref, mine_ref, group_ref):
    voc, hid = pos_ref[0], pos_ref[1]
    nv = mine_ref.shape[0]
    top = functools.reduce(jnp.maximum, [mine_ref[v, 0:1] for v in range(nv)])
    total = at_tgt = below = jnp.zeros_like(top)
    for v in range(nv):
        f = jnp.exp(mine_ref[v, 0:1] - top)
        s = mine_ref[v, 1:2] * f
        total += s
        at_tgt += mine_ref[v, 2:3] * f
        below += jnp.where((v < voc) | ((v == voc) & (hid == 0)), s, 0.0)
    row = lax.broadcasted_iota(jnp.int32, group_ref.shape, 0)
    group_ref[...] = jnp.where(row == 0, top, jnp.where(row == 1, total, jnp.where(row == 2, at_tgt, below)))


def group_stats(pos, mine):
    return pl.pallas_call(
        group_kernel,
        out_shape=jax.ShapeDtypeStruct(mine.shape[1:], jnp.float32),
        grid_spec=pltpu.PrefetchScalarGridSpec(
            num_scalar_prefetch=1,
            grid=(1,),
            in_specs=[pl.BlockSpec(mine.shape, lambda i, s: (0, 0, 0))],
            out_specs=pl.BlockSpec(mine.shape[1:], lambda i, s: (0, 0)),
        ),
        compiler_params=pltpu.CompilerParams(dimension_semantics=("arbitrary",), vmem_limit_bytes=ALL_VMEM),
        name="group_stats",
    )(pos, mine)


def merged(ct, at_tgt, blk, at, rows):
    row = lax.broadcasted_iota(jnp.int32, ct.shape, 0)
    lane = lax.broadcasted_iota(jnp.int32, ct.shape, 1)
    return jnp.where((row == blk) & (lane >= at) & (lane < at + rows), at_tgt, ct)


def final_kernel(pos_ref, pre_ref, st_ref, mine_ref, other_ref, ctin_ref, *refs, blk, at, rows):
    out_ref, ct_ref, ab_s = refs[-3:]
    step = pl.program_id(0)
    sub = pre_ref.shape[0]

    @pl.when(step == 0)
    def _():
        voc = pos_ref[0]
        own = st_ref[...]
        others = []
        row = lax.broadcasted_iota(jnp.int32, own.shape, 0)
        for v in range(mine_ref.shape[0]):
            st = jnp.where((row == 0) | (v != voc), mine_ref[v], 0.0)
            others.append((st, jnp.where(v < voc, st[1:2], 0.0)))
        others.append((other_ref[...], other_ref[3:4]))
        ab, at_tgt = combine(own, others)
        ab_s[...] = ab
        ct_ref[...] = merged(ctin_ref[...], at_tgt, blk, at, rows)

    ab = ab_s[pl.ds(pl.multiple_of(at + step * sub, sub), sub), :]
    out_ref[...] = pre_ref[...] * ab[:, 0:1] + ab[:, 1:2]


def finish(pos, pre, st, mine, other, out, ct, all_rows, blk, at, row0, deps):
    rows, cols = pre.shape
    sub = math.gcd(SUB, rows, at)
    tail = ([] if out is None else [out]) + list(deps)
    small = pl.BlockSpec((8, 128), lambda i, s: (0, 0))
    wide = pl.BlockSpec(mine.shape, lambda i, s: (0, 0, 0))
    return pl.pallas_call(
        functools.partial(final_kernel, blk=blk, at=at, rows=rows),
        out_shape=[jax.ShapeDtypeStruct((all_rows, cols), jnp.float32), jax.ShapeDtypeStruct((8, 128), jnp.float32)],
        grid_spec=pltpu.PrefetchScalarGridSpec(
            num_scalar_prefetch=1,
            grid=(rows // sub,),
            in_specs=[pl.BlockSpec((sub, cols), lambda i, s: (i, 0)), small, wide, small, small]
            + [pl.BlockSpec(memory_space=pl.ANY)] * len(tail),
            out_specs=[pl.BlockSpec((sub, cols), lambda i, s: (row0 // sub + i, 0)), small],
            scratch_shapes=[pltpu.VMEM((128, 128), jnp.float32)],
        ),
        input_output_aliases={} if out is None else {6: 0},
        cost_estimate=pl.CostEstimate(flops=64 * rows * cols, bytes_accessed=rows * cols * 8, transcendentals=0),
        compiler_params=pltpu.CompilerParams(dimension_semantics=("arbitrary",), vmem_limit_bytes=ALL_VMEM),
    )(pos, pre, st, mine, other, ct, *tail)


def last_kernel(ab_ref, at_tgt_ref, ctin_ref, *refs, blk, at, rows, ends):
    out_ref, ct_ref = refs[-2:]
    step = pl.program_id(0)
    sub = out_ref.shape[0]
    ab = ab_ref[pl.ds(pl.multiple_of(at + step * sub, sub), sub), :]
    ct_ref[...] = merged(ctin_ref[...], at_tgt_ref[...], blk, at, rows)
    for i, (lo, hi) in enumerate(ends):
        @pl.when((step >= lo) & (step < hi))
        def _(pre_ref=refs[i]):
            out_ref[...] = pre_ref[...] * ab[:, 0:1] + ab[:, 1:2]


def finish_last(ab, at_tgt, ct, pres, out, blk, at, row0, deps):
    cols = out.shape[1]
    rows = [p.shape[0] for p in pres]
    sub = math.gcd(*rows)
    ends, lo = [], 0
    for r in rows:
        ends.append((lo, lo + r // sub))
        lo += r // sub
    small = pl.BlockSpec((8, 128), lambda i: (0, 0))
    return pl.pallas_call(
        functools.partial(last_kernel, blk=blk, at=at, rows=sum(rows), ends=tuple(ends)),
        grid=(lo,),
        out_shape=[jax.ShapeDtypeStruct(out.shape, jnp.float32), jax.ShapeDtypeStruct((8, 128), jnp.float32)],
        in_specs=[pl.BlockSpec((128, 128), lambda i: (0, 0)), small, small]
        + [pl.BlockSpec((sub, cols), lambda i, lo=lo, hi=hi: (jnp.clip(i - lo, 0, hi - lo - 1), 0)) for lo, hi in ends]
        + [pl.BlockSpec(memory_space=pl.ANY)] * (1 + len(deps)),
        out_specs=[pl.BlockSpec((sub, cols), lambda i: (row0 // sub + i, 0)), small],
        input_output_aliases={3 + len(pres): 0},
        compiler_params=pltpu.CompilerParams(dimension_semantics=("arbitrary",), vmem_limit_bytes=ALL_VMEM),
        name="finish_last",
    )(ab, at_tgt, ct, *pres, out, *deps)


def solution(mesh):
    def pipeline(h, w, temp, tgt):
        rows_all = h.shape[0]
        cols = w.shape[1] // 2
        hid = lax.axis_index("hid")
        voc = lax.axis_index("vocab")
        own_half = hid.astype(jnp.int32).reshape(1)
        peer_half = (1 - hid).astype(jnp.int32).reshape(1)
        pos = jnp.stack([voc, hid]).astype(jnp.int32)
        temp2 = temp[:, None]
        tgt2 = (tgt - (voc * 2 + hid) * cols)[:, None]
        tri = (lax.broadcasted_iota(jnp.int32, (CT, CT), 0) <= lax.broadcasted_iota(jnp.int32, (CT, CT), 1)).astype(jnp.bfloat16)
        swap = [(0, 1), (1, 0)]

        blk = 128
        nblk = rows_all // blk
        last = (32, 48, 32, 16)
        tn = 7 * CT
        ht = cols // tn

        units = [(b, 0, blk) for b in range(nblk - 1)]
        units += [(nblk - 1, sum(last[:i]), r) for i, r in enumerate(last)]
        nu = len(units)
        parts = {}
        owns = {}
        tok = None

        def peer(b):
            nonlocal tok
            if b >= nblk:
                return
            splits = last if b == nblk - 1 else (blk,)
            outs = partial_products(h, w, peer_half, b * blk, splits, 0, ht, tn, ht, (tok,))
            tok = outs[0]
            for i, o in enumerate(outs):
                parts[b + i] = [o]

        def mine_half(b):
            nonlocal tok
            if b >= nblk:
                return
            tok = owns[b] = partial_products(h, w, own_half, b * blk, (blk,), 0, ht, tn, ht, (tok,))[0]

        at = 0
        parts[0] = []
        for i, n in enumerate((1, 4, 2 * ht - 5)):
            tok = partial_products(
                h, w, peer_half, 0, (blk,), at, n, tn // 2, 2 * ht, () if i == 0 else (tok,),
                2 if i == 0 else 1)[0]
            parts[0].append(tok)
            at += n
        peer(1)
        peer(2)
        mine_half(0)
        mine_half(1)

        def send(arrays):
            return [lax.ppermute(a, "hid", swap) for a in arrays]

        recvs = {0: [send([p])[0] for p in parts[0]], 1: send(parts[1])}
        pres, stats = {}, {}
        out = None
        ct = jnp.zeros((nblk, blk), jnp.float32)

        def close(k):
            nonlocal out, ct, tok
            b, at, _ = units[k]
            out, ct = finish(pos, pres[k], *stats[k], out, ct, rows_all, b, at, b * blk + at, (tok,))
            tok = ct

        prev = None
        for k, (b, at, rows) in enumerate(units):
            share = k == nu - 1
            pres[k], *small = local_prefix(
                temp2, tgt2, tri, owns[b], at, recvs[k], rows, b * blk + at, prev, (tok,), share)
            if share:
                at = units[k - 1][1]
                out, ct = finish_last(*small, ct, [pres[k - 1], pres[k]], out, b, at, b * blk + at, (tok,))
                break
            tok = st = small[0]
            if k == nu - 2:
                prev = st
                close(k - 1)
                continue
            mine = lax.all_gather(st, "vocab")
            grp = group_stats(pos, mine)
            *sent, grp = lax.optimization_barrier((*parts[k + 2], grp))
            stats[k] = (st, mine, send([grp])[0])
            recvs[k + 2] = send(sent)
            tok = grp
            if k >= 1:
                close(k - 1)
            peer(k + 3)
            mine_half(k + 2)
        return out, ct.reshape(rows_all)

    return jax.shard_map(
        pipeline,
        mesh=mesh,
        in_specs=(P("data", "hid"), P("hid", "vocab"), P("data"), P("data")),
        out_specs=(P("data", ("vocab", "hid")), P("data")),
        check_vma=False,
    )
```

```python
import functools
import math

import jax
import jax.numpy as jnp
from jax import lax
from jax.experimental import pallas as pl
from jax.experimental.pallas import tpu as pltpu
from jax.sharding import PartitionSpec as P


CT = 256
SUB = 32
LAST_VMEM = 67043328 - 9 * 512 * 1024
ALL_VMEM = 67043328


def mm_kernel(sel_ref, h_ref, w_ref, *refs, splits, ksteps):
    out_refs = refs[len(refs) - len(splits):]
    res = jnp.dot(h_ref[...], w_ref[...], preferred_element_type=jnp.float32)

    def put(add):
        at = 0
        for ref, rows in zip(out_refs, splits):
            ref[...] = ref[...] + res[at:at + rows] if add else res[at:at + rows]
            at += rows

    if ksteps == 1:
        put(False)
    else:
        pl.when(pl.program_id(1) == 0)(functools.partial(put, False))
        pl.when(pl.program_id(1) > 0)(functools.partial(put, True))


def partial_products(h, w, half, row0, splits, tile0, ntiles, tn, half_tiles, deps=(), ksteps=1):
    rows = sum(splits)
    depth = h.shape[1]
    cols = ntiles * tn
    return pl.pallas_call(
        functools.partial(mm_kernel, splits=splits, ksteps=ksteps),
        out_shape=[jax.ShapeDtypeStruct((r, cols), jnp.float32) for r in splits],
        grid_spec=pltpu.PrefetchScalarGridSpec(
            num_scalar_prefetch=1,
            grid=(ntiles, ksteps),
            in_specs=[
                pl.BlockSpec((rows, depth // ksteps), lambda j, k, s: (row0 // rows, k)),
                pl.BlockSpec((depth // ksteps, tn), lambda j, k, s: (k, s[0] * half_tiles + tile0 + j)),
            ] + [pl.BlockSpec(memory_space=pl.ANY)] * len(deps),
            out_specs=[pl.BlockSpec((r, tn), lambda j, k, s: (0, j)) for r in splits],
        ),
        cost_estimate=pl.CostEstimate(
            flops=2 * rows * depth * cols, bytes_accessed=depth * cols * 2 + rows * cols * 4, transcendentals=0),
        compiler_params=pltpu.CompilerParams(dimension_semantics=("arbitrary", "arbitrary"), vmem_limit_bytes=ALL_VMEM),
    )(half, h, w, *deps)


def local_kernel(temp_ref, tgt_ref, tri_ref, own_ref, *refs, npieces, has_prev, skip, at, group, share, keep):
    recv_refs = refs[:npieces]
    prev_ref = refs[npieces] if has_prev else None
    if share:
        pre_ref, ab_ref, at_tgt_ref, z_s, hi_s, mid_s, lo_s, st_s, st_ref, slots, send_sem, recv_sem = refs[npieces + has_prev + skip:]
        announce()
    else:
        pre_ref, st_ref, z_s, hi_s, mid_s, lo_s, st_s = refs[npieces + has_prev + skip:]
    step, nsteps = pl.program_id(0), pl.num_programs(0)
    rows = own_ref.shape[0]
    nt = own_ref.shape[1] // CT
    temp = jnp.broadcast_to(temp_ref[...], (rows, CT))
    mx = jnp.full((rows, CT), -jnp.inf, jnp.float32)

    def add_tile(t, part, mx):
        z = (own_ref[:, pl.ds(pl.multiple_of(t * CT, CT), CT)] + part) * temp
        z_s[t] = z
        return jnp.maximum(mx, z)

    t0 = off = 0
    for i, ref in enumerate(recv_refs):
        n, rest = divmod(ref.shape[1] - off, CT)

        def max_step(j, mx, ref=ref, t0=t0, off=off):
            return add_tile(t0 + j, ref[:, pl.ds(pl.multiple_of(off + j * CT, 128), CT)], mx)

        mx = lax.fori_loop(0, n, max_step, mx, unroll=max(u for u in range(1, 8) if n % u == 0))
        t0, off = t0 + n, 0
        if rest:
            off = CT - rest
            both = jnp.concatenate([ref[:, ref.shape[1] - rest:], recv_refs[i + 1][:, :off]], axis=1)
            mx = add_tile(t0, both, mx)
            t0 += 1
    m = jnp.max(mx, axis=1, keepdims=True)
    mb = jnp.broadcast_to(m, (rows, CT))
    tgt = jnp.broadcast_to(tgt_ref[...], (rows, CT))
    col = lax.broadcasted_iota(jnp.int32, (rows, CT), 1)
    rel = tgt - col

    def exp_step(j, carry):
        sacc, cacc = carry
        e = jnp.exp(z_s[j] - mb)
        hi = e.astype(jnp.bfloat16)
        r1 = e - hi.astype(jnp.float32)
        mid = r1.astype(jnp.bfloat16)
        lo = (r1 - mid.astype(jnp.float32)).astype(jnp.bfloat16)
        hi_s[j] = hi
        mid_s[j] = mid
        lo_s[j] = lo
        return sacc + e, cacc + jnp.where(rel >= j * CT, e, 0.0)

    zero = jnp.zeros((rows, CT), jnp.float32)
    sacc, cacc = lax.fori_loop(0, nt, exp_step, (zero, zero), unroll=7)
    s = jnp.sum(sacc, axis=1, keepdims=True)
    c = jnp.sum(cacc, axis=1, keepdims=True)
    lane = lax.broadcasted_iota(jnp.int32, (rows, 128), 1)

    @pl.when(step == 0)
    def _():
        st_s[...] = jnp.zeros_like(st_s)

    st_s[pl.ds(pl.multiple_of(at + step * rows, rows), rows), :] = jnp.where(
        lane == 0, m, jnp.where(lane == 1, s, jnp.where(lane == 2, c, 0.0)))

    @pl.when(step == nsteps - 1)
    def _():
        st = st_s[...].T[0:8]
        st_ref[...] = st + prev_ref[...] if has_prev else st

    if share:
        copies = spread(st_ref, slots, send_sem, recv_sem)
    tri = tri_ref[...]
    out_rows = pl.ds(pl.multiple_of(step * rows, rows), rows) if keep else slice(None)

    def prefix_step(g, carry):
        span = pl.ds(g * group, group)
        pre = jnp.dot(hi_s[span].reshape(group * rows, CT), tri, preferred_element_type=jnp.float32)
        pre += jnp.dot(mid_s[span].reshape(group * rows, CT), tri, preferred_element_type=jnp.float32)
        pre += jnp.dot(lo_s[span].reshape(group * rows, CT), tri, preferred_element_type=jnp.float32)
        for k in range(group):
            blk = pre[k * rows:(k + 1) * rows]
            dst = pl.ds(pl.multiple_of((g * group + k) * CT, CT), CT)
            pre_ref[out_rows, dst] = blk + carry
            carry = carry + jnp.broadcast_to(blk[:, CT - 1:CT], (rows, CT))
        return carry

    lax.fori_loop(0, nt // group, prefix_step, zero)
    if share:
        gather(copies, st_ref, slots, ab_ref, at_tgt_ref)


def local_prefix(temp, tgt, tri, own, at, recvs, rows, row0, prev, deps, share=False, keep=False):
    cols = own.shape[1]
    nt = cols // CT
    sub = math.gcd(SUB, rows, at)
    small = (128, 8) if share else (8,)
    vmem = pl.BlockSpec(memory_space=pltpu.VMEM)
    extra = ([] if prev is None else [prev]) + list(deps)
    extra_specs = ([] if prev is None else [pl.BlockSpec((8, 128), lambda i: (0, 0))])
    extra_specs += [pl.BlockSpec(memory_space=pl.ANY)] * len(deps)
    return pl.pallas_call(
        functools.partial(
            local_kernel, npieces=len(recvs), has_prev=int(prev is not None), skip=len(deps), at=at, group=7 if sub > 16 else 49,
            share=share, keep=keep),
        grid=(rows // sub,),
        out_shape=[(pltpu.VMEM if keep else jax.ShapeDtypeStruct)((rows, cols), jnp.float32)]
        + [(pltpu.VMEM if share else jax.ShapeDtypeStruct)((n, 128), jnp.float32) for n in small],
        in_specs=[
            pl.BlockSpec((sub, 1), lambda i: (row0 // sub + i, 0)),
            pl.BlockSpec((sub, 1), lambda i: (row0 // sub + i, 0)),
            pl.BlockSpec((CT, CT), lambda i: (0, 0)),
            pl.BlockSpec((sub, cols), lambda i: (at // sub + i, 0)),
        ] + [pl.BlockSpec((sub, r.shape[1]), lambda i: (i, 0)) for r in recvs] + extra_specs,
        out_specs=[vmem if keep else pl.BlockSpec((sub, cols), lambda i: (i, 0))]
        + ([vmem, vmem] if share else [pl.BlockSpec((8, 128), lambda i: (0, 0))]),
        scratch_shapes=[
            pltpu.VMEM((nt, sub, CT), jnp.float32),
            pltpu.VMEM((nt, sub, CT), jnp.bfloat16),
            pltpu.VMEM((nt, sub, CT), jnp.bfloat16),
            pltpu.VMEM((nt, sub, CT), jnp.bfloat16),
            pltpu.VMEM((128, 128), jnp.float32),
        ] + ([
            pltpu.VMEM((8, 128), jnp.float32),
            pltpu.VMEM((7, 8, 128), jnp.float32),
            pltpu.SemaphoreType.DMA((7,)),
            pltpu.SemaphoreType.DMA((7,)),
        ] if share else []),
        cost_estimate=pl.CostEstimate(
            flops=6 * rows * cols * CT, bytes_accessed=rows * cols * 12, transcendentals=rows * cols),
        compiler_params=pltpu.CompilerParams(
            dimension_semantics=("arbitrary",), vmem_limit_bytes=LAST_VMEM if keep else ALL_VMEM,
            **(dict(collective_id=0, has_side_effects=True) if share else {})),
    )(temp, tgt, tri, own, *recvs, *extra)


STEPS = [(dv, dh) for dv in range(4) for dh in range(2)][1:]


def device(dv, dh):
    return {"vocab": lax.rem(lax.axis_index("vocab") + dv, 4), "hid": lax.rem(lax.axis_index("hid") + dh, 2)}


def announce():
    barrier = pltpu.get_barrier_semaphore()
    for dv, dh in STEPS:
        pl.semaphore_signal(barrier, inc=1, device_id=device(dv, dh), device_id_type=pl.DeviceIdType.MESH)


def spread(st_ref, slots, send_sem, recv_sem):
    pl.semaphore_wait(pltpu.get_barrier_semaphore(), len(STEPS))
    copies = []
    for i, (dv, dh) in enumerate(STEPS):
        copy = pltpu.make_async_remote_copy(
            src_ref=st_ref,
            dst_ref=slots.at[i],
            send_sem=send_sem.at[i],
            recv_sem=recv_sem.at[i],
            device_id=device(dv, dh),
            device_id_type=pl.DeviceIdType.MESH,
        )
        copy.start()
        copies.append(copy)
    return copies


def gather(copies, st_ref, slots, ab_ref, at_tgt_ref):
    for copy in copies:
        copy.wait()
    voc = lax.axis_index("vocab")
    hid = lax.axis_index("hid")
    me = voc * 2 + hid
    stats = []
    for i, (dv, dh) in enumerate(STEPS):
        index = lax.rem(voc + 4 - dv, 4) * 2 + lax.rem(hid + 2 - dh, 2)
        st = slots[i]
        stats.append((st, jnp.where(index < me, st[1:2], 0.0)))
    ab, at_tgt = combine(st_ref[...], stats)
    ab_ref[...] = ab
    at_tgt_ref[...] = jnp.broadcast_to(at_tgt, at_tgt_ref.shape)


def combine(own, others):
    top = functools.reduce(jnp.maximum, [st[0:1] for st, _ in others], own[0:1])
    scale = jnp.exp(own[0:1] - top)
    total = own[1:2] * scale
    at_tgt = own[2:3] * scale
    below = jnp.zeros_like(top)
    for st, lower in others:
        f = jnp.exp(st[0:1] - top)
        total += st[1:2] * f
        at_tgt += st[2:3] * f
        below += lower * f
    inv = 1.0 / total
    first = lax.broadcasted_iota(jnp.int32, (128, 128), 0) == 0
    return jnp.where(first, scale * inv, below * inv).T, at_tgt * inv


def group_kernel(pos_ref, mine_ref, group_ref):
    voc, hid = pos_ref[0], pos_ref[1]
    nv = mine_ref.shape[0]
    top = functools.reduce(jnp.maximum, [mine_ref[v, 0:1] for v in range(nv)])
    total = at_tgt = below = jnp.zeros_like(top)
    for v in range(nv):
        f = jnp.exp(mine_ref[v, 0:1] - top)
        s = mine_ref[v, 1:2] * f
        total += s
        at_tgt += mine_ref[v, 2:3] * f
        below += jnp.where((v < voc) | ((v == voc) & (hid == 0)), s, 0.0)
    row = lax.broadcasted_iota(jnp.int32, group_ref.shape, 0)
    group_ref[...] = jnp.where(row == 0, top, jnp.where(row == 1, total, jnp.where(row == 2, at_tgt, below)))


def group_stats(pos, mine):
    return pl.pallas_call(
        group_kernel,
        out_shape=jax.ShapeDtypeStruct(mine.shape[1:], jnp.float32),
        grid_spec=pltpu.PrefetchScalarGridSpec(
            num_scalar_prefetch=1,
            grid=(1,),
            in_specs=[pl.BlockSpec(mine.shape, lambda i, s: (0, 0, 0))],
            out_specs=pl.BlockSpec(mine.shape[1:], lambda i, s: (0, 0)),
        ),
        compiler_params=pltpu.CompilerParams(dimension_semantics=("arbitrary",), vmem_limit_bytes=ALL_VMEM),
        name="group_stats",
    )(pos, mine)


def merged(ct, at_tgt, blk, at, rows):
    row = lax.broadcasted_iota(jnp.int32, ct.shape, 0)
    lane = lax.broadcasted_iota(jnp.int32, ct.shape, 1)
    return jnp.where((row == blk) & (lane >= at) & (lane < at + rows), at_tgt, ct)


def final_kernel(pos_ref, pre_ref, st_ref, mine_ref, other_ref, ctin_ref, *refs, blk, at, rows):
    out_ref, ct_ref, ab_s = refs[-3:]
    step = pl.program_id(0)
    sub = pre_ref.shape[0]

    @pl.when(step == 0)
    def _():
        voc = pos_ref[0]
        own = st_ref[...]
        others = []
        row = lax.broadcasted_iota(jnp.int32, own.shape, 0)
        for v in range(mine_ref.shape[0]):
            st = jnp.where((row == 0) | (v != voc), mine_ref[v], 0.0)
            others.append((st, jnp.where(v < voc, st[1:2], 0.0)))
        others.append((other_ref[...], other_ref[3:4]))
        ab, at_tgt = combine(own, others)
        ab_s[...] = ab
        ct_ref[...] = merged(ctin_ref[...], at_tgt, blk, at, rows)

    ab = ab_s[pl.ds(pl.multiple_of(at + step * sub, sub), sub), :]
    out_ref[...] = pre_ref[...] * ab[:, 0:1] + ab[:, 1:2]


def finish(pos, pre, st, mine, other, out, ct, all_rows, blk, at, row0, deps, vmem):
    rows, cols = pre.shape
    sub = math.gcd(SUB, rows, at)
    tail = ([] if out is None else [out]) + list(deps)
    small = pl.BlockSpec((8, 128), lambda i, s: (0, 0))
    wide = pl.BlockSpec(mine.shape, lambda i, s: (0, 0, 0))
    return pl.pallas_call(
        functools.partial(final_kernel, blk=blk, at=at, rows=rows),
        out_shape=[jax.ShapeDtypeStruct((all_rows, cols), jnp.float32), jax.ShapeDtypeStruct((8, 128), jnp.float32)],
        grid_spec=pltpu.PrefetchScalarGridSpec(
            num_scalar_prefetch=1,
            grid=(rows // sub,),
            in_specs=[pl.BlockSpec((sub, cols), lambda i, s: (i, 0)), small, wide, small, small]
            + [pl.BlockSpec(memory_space=pl.ANY)] * len(tail),
            out_specs=[pl.BlockSpec((sub, cols), lambda i, s: (row0 // sub + i, 0)), small],
            scratch_shapes=[pltpu.VMEM((128, 128), jnp.float32)],
        ),
        input_output_aliases={} if out is None else {6: 0},
        cost_estimate=pl.CostEstimate(flops=64 * rows * cols, bytes_accessed=rows * cols * 8, transcendentals=0),
        compiler_params=pltpu.CompilerParams(dimension_semantics=("arbitrary",), vmem_limit_bytes=vmem),
    )(pos, pre, st, mine, other, ct, *tail)


def last_kernel(ab_ref, at_tgt_ref, ctin_ref, *refs, blk, at, rows, ends):
    out_ref, ct_ref = refs[-2:]
    step = pl.program_id(0)
    sub = out_ref.shape[0]
    ab = ab_ref[pl.ds(pl.multiple_of(at + step * sub, sub), sub), :]
    ct_ref[...] = merged(ctin_ref[...], at_tgt_ref[...], blk, at, rows)
    for i, (lo, hi) in enumerate(ends):
        @pl.when((step >= lo) & (step < hi))
        def _(pre_ref=refs[i], lo=lo):
            here = pl.ds(pl.multiple_of((step - lo) * sub, sub), sub)
            out_ref[...] = pre_ref[here, :] * ab[:, 0:1] + ab[:, 1:2]


def held(x):
    return pltpu.with_memory_space_constraint(x, pltpu.VMEM)


def finish_last(ab, at_tgt, ct, pres, out, blk, at, row0, deps):
    cols = out.shape[1]
    rows = [p.shape[0] for p in pres]
    sub = math.gcd(*rows)
    ends, lo = [], 0
    for r in rows:
        ends.append((lo, lo + r // sub))
        lo += r // sub
    whole = pl.BlockSpec(memory_space=pltpu.VMEM)
    small = pl.BlockSpec((8, 128), lambda i: (0, 0))
    return pl.pallas_call(
        functools.partial(last_kernel, blk=blk, at=at, rows=sum(rows), ends=tuple(ends)),
        grid=(lo,),
        out_shape=[jax.ShapeDtypeStruct(out.shape, jnp.float32), jax.ShapeDtypeStruct((8, 128), jnp.float32)],
        in_specs=[whole, whole, small]
        + [whole] * len(pres)
        + [pl.BlockSpec(memory_space=pl.ANY)] * (1 + len(deps)),
        out_specs=[pl.BlockSpec((sub, cols), lambda i: (row0 // sub + i, 0)), small],
        input_output_aliases={3 + len(pres): 0},
        compiler_params=pltpu.CompilerParams(dimension_semantics=("arbitrary",), vmem_limit_bytes=LAST_VMEM),
        name="finish_last",
    )(held(ab), held(at_tgt), ct, *map(held, pres), out, *deps)


def solution(mesh):
    def pipeline(h, w, temp, tgt):
        rows_all = h.shape[0]
        cols = w.shape[1] // 2
        hid = lax.axis_index("hid")
        voc = lax.axis_index("vocab")
        own_half = hid.astype(jnp.int32).reshape(1)
        peer_half = (1 - hid).astype(jnp.int32).reshape(1)
        pos = jnp.stack([voc, hid]).astype(jnp.int32)
        temp2 = temp[:, None]
        tgt2 = (tgt - (voc * 2 + hid) * cols)[:, None]
        tri = (lax.broadcasted_iota(jnp.int32, (CT, CT), 0) <= lax.broadcasted_iota(jnp.int32, (CT, CT), 1)).astype(jnp.bfloat16)
        swap = [(0, 1), (1, 0)]

        blk = 128
        nblk = rows_all // blk
        last = (32, 48, 32, 16)
        tn = 7 * CT
        ht = cols // tn

        units = [(b, 0, blk) for b in range(nblk - 1)]
        units += [(nblk - 1, sum(last[:i]), r) for i, r in enumerate(last)]
        nu = len(units)
        parts = {}
        owns = {}
        tok = None

        def peer(b):
            nonlocal tok
            if b >= nblk:
                return
            splits = last if b == nblk - 1 else (blk,)
            outs = partial_products(h, w, peer_half, b * blk, splits, 0, ht, tn, ht, (tok,))
            tok = outs[0]
            for i, o in enumerate(outs):
                parts[b + i] = [o]

        def mine_half(b):
            nonlocal tok
            if b >= nblk:
                return
            tok = owns[b] = partial_products(h, w, own_half, b * blk, (blk,), 0, ht, tn, ht, (tok,))[0]

        at = 0
        parts[0] = []
        for i, n in enumerate((1, 4, 2 * ht - 5)):
            tok = partial_products(
                h, w, peer_half, 0, (blk,), at, n, tn // 2, 2 * ht, () if i == 0 else (tok,),
                2 if i == 0 else 1)[0]
            parts[0].append(tok)
            at += n
        peer(1)
        peer(2)
        mine_half(0)
        mine_half(1)

        def send(arrays):
            return [lax.ppermute(a, "hid", swap) for a in arrays]

        recvs = {0: [send([p])[0] for p in parts[0]], 1: send(parts[1])}
        pres, stats = {}, {}
        out = None
        ct = jnp.zeros((nblk, blk), jnp.float32)

        def close(k):
            nonlocal out, ct, tok
            b, at, _ = units[k]
            out, ct = finish(pos, pres[k], *stats[k], out, ct, rows_all, b, at, b * blk + at, (tok,),
                             LAST_VMEM if k == nu - 3 else ALL_VMEM)
            tok = ct

        prev = None
        for k, (b, at, rows) in enumerate(units):
            share = k == nu - 1
            pres[k], *small = local_prefix(
                temp2, tgt2, tri, owns[b], at, recvs[k], rows, b * blk + at, prev, (tok,), share,
                k >= nu - 2)
            if share:
                at = units[k - 1][1]
                out, ct = finish_last(*small, ct, [pres[k - 1], pres[k]], out, b, at, b * blk + at, (tok,))
                break
            tok = st = small[0]
            if k == nu - 2:
                prev = st
                close(k - 1)
                continue
            mine = lax.all_gather(st, "vocab")
            grp = group_stats(pos, mine)
            *sent, grp = lax.optimization_barrier((*parts[k + 2], grp))
            stats[k] = (st, mine, send([grp])[0])
            recvs[k + 2] = send(sent)
            tok = grp
            if k >= 1:
                close(k - 1)
            peer(k + 3)
            mine_half(k + 2)
        return out, ct.reshape(rows_all)

    return jax.shard_map(
        pipeline,
        mesh=mesh,
        in_specs=(P("data", "hid"), P("hid", "vocab"), P("data"), P("data")),
        out_specs=(P("data", ("vocab", "hid")), P("data")),
        check_vma=False,
    )
```

```python
import functools
import math

import jax
import jax.numpy as jnp
from jax import lax
from jax.experimental import pallas as pl
from jax.experimental.pallas import tpu as pltpu
from jax.sharding import PartitionSpec as P


CT = 256
SUB = 32
LAST_VMEM = 67043328 - 9 * 512 * 1024
ALL_VMEM = 67043328


def mm_kernel(sel_ref, h_ref, w_ref, *refs, splits, ksteps):
    out_refs = refs[len(refs) - len(splits):]
    res = jnp.dot(h_ref[...], w_ref[...], preferred_element_type=jnp.float32)

    def put(add):
        at = 0
        for ref, rows in zip(out_refs, splits):
            ref[...] = ref[...] + res[at:at + rows] if add else res[at:at + rows]
            at += rows

    if ksteps == 1:
        put(False)
    else:
        pl.when(pl.program_id(1) == 0)(functools.partial(put, False))
        pl.when(pl.program_id(1) > 0)(functools.partial(put, True))


def partial_products(h, w, half, row0, splits, tile0, ntiles, tn, half_tiles, deps=(), ksteps=1):
    rows = sum(splits)
    depth = h.shape[1]
    cols = ntiles * tn
    return pl.pallas_call(
        functools.partial(mm_kernel, splits=splits, ksteps=ksteps),
        out_shape=[jax.ShapeDtypeStruct((r, cols), jnp.float32) for r in splits],
        grid_spec=pltpu.PrefetchScalarGridSpec(
            num_scalar_prefetch=1,
            grid=(ntiles, ksteps),
            in_specs=[
                pl.BlockSpec((rows, depth // ksteps), lambda j, k, s: (row0 // rows, k)),
                pl.BlockSpec((depth // ksteps, tn), lambda j, k, s: (k, s[0] * half_tiles + tile0 + j)),
            ] + [pl.BlockSpec(memory_space=pl.ANY)] * len(deps),
            out_specs=[pl.BlockSpec((r, tn), lambda j, k, s: (0, j)) for r in splits],
        ),
        cost_estimate=pl.CostEstimate(
            flops=2 * rows * depth * cols, bytes_accessed=depth * cols * 2 + rows * cols * 4, transcendentals=0),
        compiler_params=pltpu.CompilerParams(dimension_semantics=("arbitrary", "arbitrary"), vmem_limit_bytes=ALL_VMEM),
    )(half, h, w, *deps)


def local_kernel(temp_ref, tgt_ref, tri_ref, own_ref, *refs, npieces, has_prev, skip, at, group, share, keep):
    recv_refs = refs[:npieces]
    prev_ref = refs[npieces] if has_prev else None
    if share:
        pre_ref, ab_ref, at_tgt_ref, z_s, hi_s, mid_s, lo_s, st_s, st_ref, slots, send_sem, recv_sem = refs[npieces + has_prev + skip:]
        announce()
    else:
        pre_ref, st_ref, z_s, hi_s, mid_s, lo_s, st_s = refs[npieces + has_prev + skip:]
    step, nsteps = pl.program_id(0), pl.num_programs(0)
    rows = own_ref.shape[0]
    nt = own_ref.shape[1] // CT
    temp = jnp.broadcast_to(temp_ref[...], (rows, CT))
    mx = jnp.full((rows, CT), -jnp.inf, jnp.float32)

    def add_tile(t, part, mx):
        z = (own_ref[:, pl.ds(pl.multiple_of(t * CT, CT), CT)] + part) * temp
        z_s[t] = z
        return jnp.maximum(mx, z)

    t0 = off = 0
    for i, ref in enumerate(recv_refs):
        n, rest = divmod(ref.shape[1] - off, CT)

        def max_step(j, mx, ref=ref, t0=t0, off=off):
            return add_tile(t0 + j, ref[:, pl.ds(pl.multiple_of(off + j * CT, 128), CT)], mx)

        mx = lax.fori_loop(0, n, max_step, mx, unroll=max(u for u in range(1, 8) if n % u == 0))
        t0, off = t0 + n, 0
        if rest:
            off = CT - rest
            both = jnp.concatenate([ref[:, ref.shape[1] - rest:], recv_refs[i + 1][:, :off]], axis=1)
            mx = add_tile(t0, both, mx)
            t0 += 1
    m = jnp.max(mx, axis=1, keepdims=True)
    mb = jnp.broadcast_to(m, (rows, CT))
    tgt = jnp.broadcast_to(tgt_ref[...], (rows, CT))
    col = lax.broadcasted_iota(jnp.int32, (rows, CT), 1)
    rel = tgt - col

    def exp_step(j, carry):
        sacc, cacc = carry
        e = jnp.exp(z_s[j] - mb)
        hi = e.astype(jnp.bfloat16)
        r1 = e - hi.astype(jnp.float32)
        mid = r1.astype(jnp.bfloat16)
        lo = (r1 - mid.astype(jnp.float32)).astype(jnp.bfloat16)
        hi_s[j] = hi
        mid_s[j] = mid
        lo_s[j] = lo
        return sacc + e, cacc + jnp.where(rel >= j * CT, e, 0.0)

    zero = jnp.zeros((rows, CT), jnp.float32)
    sacc, cacc = lax.fori_loop(0, nt, exp_step, (zero, zero), unroll=7)
    s = jnp.sum(sacc, axis=1, keepdims=True)
    c = jnp.sum(cacc, axis=1, keepdims=True)
    lane = lax.broadcasted_iota(jnp.int32, (rows, 128), 1)

    @pl.when(step == 0)
    def _():
        st_s[...] = jnp.zeros_like(st_s)

    st_s[pl.ds(pl.multiple_of(at + step * rows, rows), rows), :] = jnp.where(
        lane == 0, m, jnp.where(lane == 1, s, jnp.where(lane == 2, c, 0.0)))

    @pl.when(step == nsteps - 1)
    def _():
        st = st_s[...].T[0:8]
        st_ref[...] = st + prev_ref[...] if has_prev else st

    if share:
        copies = spread(st_ref, slots, send_sem, recv_sem)
    tri = tri_ref[...]
    out_rows = pl.ds(pl.multiple_of(step * rows, rows), rows) if keep else slice(None)

    def prefix_step(g, carry):
        span = pl.ds(g * group, group)
        pre = jnp.dot(hi_s[span].reshape(group * rows, CT), tri, preferred_element_type=jnp.float32)
        pre += jnp.dot(mid_s[span].reshape(group * rows, CT), tri, preferred_element_type=jnp.float32)
        pre += jnp.dot(lo_s[span].reshape(group * rows, CT), tri, preferred_element_type=jnp.float32)
        for k in range(group):
            blk = pre[k * rows:(k + 1) * rows]
            dst = pl.ds(pl.multiple_of((g * group + k) * CT, CT), CT)
            pre_ref[out_rows, dst] = blk + carry
            carry = carry + jnp.broadcast_to(blk[:, CT - 1:CT], (rows, CT))
        return carry

    lax.fori_loop(0, nt // group, prefix_step, zero)
    if share:
        gather(copies, st_ref, slots, ab_ref, at_tgt_ref)


def local_prefix(temp, tgt, tri, own, at, recvs, rows, row0, prev, deps, share=False, keep=False):
    cols = own.shape[1]
    nt = cols // CT
    sub = math.gcd(SUB, rows, at)
    small = (128, 8) if share else (8,)
    vmem = pl.BlockSpec(memory_space=pltpu.VMEM)
    extra = ([] if prev is None else [prev]) + list(deps)
    extra_specs = ([] if prev is None else [pl.BlockSpec((8, 128), lambda i: (0, 0))])
    extra_specs += [pl.BlockSpec(memory_space=pl.ANY)] * len(deps)
    return pl.pallas_call(
        functools.partial(
            local_kernel, npieces=len(recvs), has_prev=int(prev is not None), skip=len(deps), at=at, group=7 if sub > 16 else 49,
            share=share, keep=keep),
        grid=(rows // sub,),
        out_shape=[(pltpu.VMEM if keep else jax.ShapeDtypeStruct)((rows, cols), jnp.float32)]
        + [(pltpu.VMEM if share else jax.ShapeDtypeStruct)((n, 128), jnp.float32) for n in small],
        in_specs=[
            pl.BlockSpec((sub, 1), lambda i: (row0 // sub + i, 0)),
            pl.BlockSpec((sub, 1), lambda i: (row0 // sub + i, 0)),
            pl.BlockSpec((CT, CT), lambda i: (0, 0)),
            pl.BlockSpec((sub, cols), lambda i: (at // sub + i, 0)),
        ] + [pl.BlockSpec((sub, r.shape[1]), lambda i: (i, 0)) for r in recvs] + extra_specs,
        out_specs=[vmem if keep else pl.BlockSpec((sub, cols), lambda i: (i, 0))]
        + ([vmem, vmem] if share else [pl.BlockSpec((8, 128), lambda i: (0, 0))]),
        scratch_shapes=[
            pltpu.VMEM((nt, sub, CT), jnp.float32),
            pltpu.VMEM((nt, sub, CT), jnp.bfloat16),
            pltpu.VMEM((nt, sub, CT), jnp.bfloat16),
            pltpu.VMEM((nt, sub, CT), jnp.bfloat16),
            pltpu.VMEM((128, 128), jnp.float32),
        ] + ([
            pltpu.VMEM((8, 128), jnp.float32),
            pltpu.VMEM((7, 8, 128), jnp.float32),
            pltpu.SemaphoreType.DMA((7,)),
            pltpu.SemaphoreType.DMA((7,)),
        ] if share else []),
        cost_estimate=pl.CostEstimate(
            flops=6 * rows * cols * CT, bytes_accessed=rows * cols * 12, transcendentals=rows * cols),
        compiler_params=pltpu.CompilerParams(
            dimension_semantics=("arbitrary",), vmem_limit_bytes=LAST_VMEM if keep else ALL_VMEM,
            **(dict(collective_id=0, has_side_effects=True) if share else {})),
    )(temp, tgt, tri, own, *recvs, *extra)


STEPS = [(dv, dh) for dv in range(4) for dh in range(2)][1:]


def device(dv, dh):
    return {"vocab": lax.rem(lax.axis_index("vocab") + dv, 4), "hid": lax.rem(lax.axis_index("hid") + dh, 2)}


def announce():
    barrier = pltpu.get_barrier_semaphore()
    for dv, dh in STEPS:
        pl.semaphore_signal(barrier, inc=1, device_id=device(dv, dh), device_id_type=pl.DeviceIdType.MESH)


def spread(st_ref, slots, send_sem, recv_sem):
    pl.semaphore_wait(pltpu.get_barrier_semaphore(), len(STEPS))
    copies = []
    for i, (dv, dh) in enumerate(STEPS):
        copy = pltpu.make_async_remote_copy(
            src_ref=st_ref,
            dst_ref=slots.at[i],
            send_sem=send_sem.at[i],
            recv_sem=recv_sem.at[i],
            device_id=device(dv, dh),
            device_id_type=pl.DeviceIdType.MESH,
        )
        copy.start()
        copies.append(copy)
    return copies


def gather(copies, st_ref, slots, ab_ref, at_tgt_ref):
    for copy in copies:
        copy.wait()
    voc = lax.axis_index("vocab")
    hid = lax.axis_index("hid")
    me = voc * 2 + hid
    stats = []
    for i, (dv, dh) in enumerate(STEPS):
        index = lax.rem(voc + 4 - dv, 4) * 2 + lax.rem(hid + 2 - dh, 2)
        st = slots[i]
        stats.append((st, jnp.where(index < me, st[1:2], 0.0)))
    ab, at_tgt = combine(st_ref[...], stats)
    ab_ref[...] = ab
    at_tgt_ref[...] = jnp.broadcast_to(at_tgt, at_tgt_ref.shape)


def combine(own, others):
    top = functools.reduce(jnp.maximum, [st[0:1] for st, _ in others], own[0:1])
    scale = jnp.exp(own[0:1] - top)
    total = own[1:2] * scale
    at_tgt = own[2:3] * scale
    below = jnp.zeros_like(top)
    for st, lower in others:
        f = jnp.exp(st[0:1] - top)
        total += st[1:2] * f
        at_tgt += st[2:3] * f
        below += lower * f
    inv = 1.0 / total
    first = lax.broadcasted_iota(jnp.int32, (128, 128), 0) == 0
    return jnp.where(first, scale * inv, below * inv).T, at_tgt * inv


def group_kernel(pos_ref, mine_ref, group_ref):
    voc, hid = pos_ref[0], pos_ref[1]
    nv = mine_ref.shape[0]
    top = functools.reduce(jnp.maximum, [mine_ref[v, 0:1] for v in range(nv)])
    total = at_tgt = below = jnp.zeros_like(top)
    for v in range(nv):
        f = jnp.exp(mine_ref[v, 0:1] - top)
        s = mine_ref[v, 1:2] * f
        total += s
        at_tgt += mine_ref[v, 2:3] * f
        below += jnp.where((v < voc) | ((v == voc) & (hid == 0)), s, 0.0)
    row = lax.broadcasted_iota(jnp.int32, group_ref.shape, 0)
    group_ref[...] = jnp.where(row == 0, top, jnp.where(row == 1, total, jnp.where(row == 2, at_tgt, below)))


def group_stats(pos, mine):
    return pl.pallas_call(
        group_kernel,
        out_shape=jax.ShapeDtypeStruct(mine.shape[1:], jnp.float32),
        grid_spec=pltpu.PrefetchScalarGridSpec(
            num_scalar_prefetch=1,
            grid=(1,),
            in_specs=[pl.BlockSpec(mine.shape, lambda i, s: (0, 0, 0))],
            out_specs=pl.BlockSpec(mine.shape[1:], lambda i, s: (0, 0)),
        ),
        compiler_params=pltpu.CompilerParams(dimension_semantics=("arbitrary",), vmem_limit_bytes=ALL_VMEM),
        name="group_stats",
    )(pos, mine)


def merged(ct, at_tgt, blk, at, rows):
    row = lax.broadcasted_iota(jnp.int32, ct.shape, 0)
    lane = lax.broadcasted_iota(jnp.int32, ct.shape, 1)
    return jnp.where((row == blk) & (lane >= at) & (lane < at + rows), at_tgt, ct)


def final_kernel(pos_ref, pre_ref, st_ref, mine_ref, other_ref, ctin_ref, *refs, blk, at, rows):
    out_ref, ct_ref, ab_s = refs[-3:]
    step = pl.program_id(0)
    sub = pre_ref.shape[0]

    @pl.when(step == 0)
    def _():
        voc = pos_ref[0]
        own = st_ref[...]
        others = []
        row = lax.broadcasted_iota(jnp.int32, own.shape, 0)
        for v in range(mine_ref.shape[0]):
            st = jnp.where((row == 0) | (v != voc), mine_ref[v], 0.0)
            others.append((st, jnp.where(v < voc, st[1:2], 0.0)))
        others.append((other_ref[...], other_ref[3:4]))
        ab, at_tgt = combine(own, others)
        ab_s[...] = ab
        ct_ref[...] = merged(ctin_ref[...], at_tgt, blk, at, rows)

    ab = ab_s[pl.ds(pl.multiple_of(at + step * sub, sub), sub), :]
    out_ref[...] = pre_ref[...] * ab[:, 0:1] + ab[:, 1:2]


def finish(pos, pre, st, mine, other, out, ct, all_rows, blk, at, row0, deps, keep):
    rows, cols = pre.shape
    sub = math.gcd(SUB, rows, at)
    tail = ([] if out is None else [out]) + list(deps)
    small = pl.BlockSpec((8, 128), lambda i, s: (0, 0))
    wide = pl.BlockSpec(mine.shape, lambda i, s: (0, 0, 0))
    return pl.pallas_call(
        functools.partial(final_kernel, blk=blk, at=at, rows=rows),
        out_shape=[jax.ShapeDtypeStruct((all_rows, cols), jnp.float32),
                   (pltpu.VMEM if keep else jax.ShapeDtypeStruct)((8, 128), jnp.float32)],
        grid_spec=pltpu.PrefetchScalarGridSpec(
            num_scalar_prefetch=1,
            grid=(rows // sub,),
            in_specs=[pl.BlockSpec((sub, cols), lambda i, s: (i, 0)), small, wide, small, small]
            + [pl.BlockSpec(memory_space=pl.ANY)] * len(tail),
            out_specs=[pl.BlockSpec((sub, cols), lambda i, s: (row0 // sub + i, 0)),
                       pl.BlockSpec(memory_space=pltpu.VMEM) if keep else small],
            scratch_shapes=[pltpu.VMEM((128, 128), jnp.float32)],
        ),
        input_output_aliases={} if out is None else {6: 0},
        cost_estimate=pl.CostEstimate(flops=64 * rows * cols, bytes_accessed=rows * cols * 8, transcendentals=0),
        compiler_params=pltpu.CompilerParams(dimension_semantics=("arbitrary",), vmem_limit_bytes=LAST_VMEM if keep else ALL_VMEM),
    )(pos, pre, st, mine, other, ct, *tail)


def last_kernel(ab_ref, at_tgt_ref, ctin_ref, *refs, blk, at, rows, ends):
    out_ref, ct_ref = refs[-2:]
    step = pl.program_id(0)
    sub = out_ref.shape[0]
    ab = ab_ref[pl.ds(pl.multiple_of(at + step * sub, sub), sub), :]
    ct_ref[...] = merged(ctin_ref[...], at_tgt_ref[...], blk, at, rows)
    for i, (lo, hi) in enumerate(ends):
        @pl.when((step >= lo) & (step < hi))
        def _(pre_ref=refs[i], lo=lo):
            here = pl.ds(pl.multiple_of((step - lo) * sub, sub), sub)
            out_ref[...] = pre_ref[here, :] * ab[:, 0:1] + ab[:, 1:2]


def held(x):
    return pltpu.with_memory_space_constraint(x, pltpu.VMEM)


def finish_last(ab, at_tgt, ct, pres, out, blk, at, row0, deps):
    cols = out.shape[1]
    rows = [p.shape[0] for p in pres]
    sub = math.gcd(*rows)
    ends, lo = [], 0
    for r in rows:
        ends.append((lo, lo + r // sub))
        lo += r // sub
    whole = pl.BlockSpec(memory_space=pltpu.VMEM)
    small = pl.BlockSpec((8, 128), lambda i: (0, 0))
    return pl.pallas_call(
        functools.partial(last_kernel, blk=blk, at=at, rows=sum(rows), ends=tuple(ends)),
        grid=(lo,),
        out_shape=[jax.ShapeDtypeStruct(out.shape, jnp.float32), jax.ShapeDtypeStruct((8, 128), jnp.float32)],
        in_specs=[whole, whole, whole]
        + [whole] * len(pres)
        + [pl.BlockSpec(memory_space=pl.ANY)] * (1 + len(deps)),
        out_specs=[pl.BlockSpec((sub, cols), lambda i: (row0 // sub + i, 0)), small],
        input_output_aliases={3 + len(pres): 0},
        compiler_params=pltpu.CompilerParams(dimension_semantics=("arbitrary",), vmem_limit_bytes=LAST_VMEM),
        name="finish_last",
    )(held(ab), held(at_tgt), held(ct), *map(held, pres), out, *deps)


def solution(mesh):
    def pipeline(h, w, temp, tgt):
        rows_all = h.shape[0]
        cols = w.shape[1] // 2
        hid = lax.axis_index("hid")
        voc = lax.axis_index("vocab")
        own_half = hid.astype(jnp.int32).reshape(1)
        peer_half = (1 - hid).astype(jnp.int32).reshape(1)
        pos = jnp.stack([voc, hid]).astype(jnp.int32)
        temp2 = temp[:, None]
        tgt2 = (tgt - (voc * 2 + hid) * cols)[:, None]
        tri = (lax.broadcasted_iota(jnp.int32, (CT, CT), 0) <= lax.broadcasted_iota(jnp.int32, (CT, CT), 1)).astype(jnp.bfloat16)
        swap = [(0, 1), (1, 0)]

        blk = 128
        nblk = rows_all // blk
        last = (32, 48, 32, 16)
        tn = 7 * CT
        ht = cols // tn

        units = [(b, 0, blk) for b in range(nblk - 1)]
        units += [(nblk - 1, sum(last[:i]), r) for i, r in enumerate(last)]
        nu = len(units)
        parts = {}
        owns = {}
        tok = None

        def peer(b):
            nonlocal tok
            if b >= nblk:
                return
            splits = last if b == nblk - 1 else (blk,)
            outs = partial_products(h, w, peer_half, b * blk, splits, 0, ht, tn, ht, (tok,))
            tok = outs[0]
            for i, o in enumerate(outs):
                parts[b + i] = [o]

        def mine_half(b):
            nonlocal tok
            if b >= nblk:
                return
            tok = owns[b] = partial_products(h, w, own_half, b * blk, (blk,), 0, ht, tn, ht, (tok,))[0]

        at = 0
        parts[0] = []
        for i, n in enumerate((1, 4, 2 * ht - 5)):
            tok = partial_products(
                h, w, peer_half, 0, (blk,), at, n, tn // 2, 2 * ht, () if i == 0 else (tok,),
                2 if i == 0 else 1)[0]
            parts[0].append(tok)
            at += n
        peer(1)
        peer(2)
        mine_half(0)
        mine_half(1)

        def send(arrays):
            return [lax.ppermute(a, "hid", swap) for a in arrays]

        recvs = {0: [send([p])[0] for p in parts[0]], 1: send(parts[1])}
        pres, stats = {}, {}
        out = None
        ct = jnp.zeros((nblk, blk), jnp.float32)

        def close(k):
            nonlocal out, ct, tok
            b, at, _ = units[k]
            out, ct = finish(pos, pres[k], *stats[k], out, ct, rows_all, b, at, b * blk + at, (tok,),
                             k == nu - 3)
            if k == nu - 3:
                ct = held(ct)
            tok = ct

        prev = None
        for k, (b, at, rows) in enumerate(units):
            share = k == nu - 1
            pres[k], *small = local_prefix(
                temp2, tgt2, tri, owns[b], at, recvs[k], rows, b * blk + at, prev, (tok,), share,
                k >= nu - 2)
            if share:
                at = units[k - 1][1]
                out, ct = finish_last(*small, ct, [pres[k - 1], pres[k]], out, b, at, b * blk + at, (tok,))
                break
            tok = st = small[0]
            if k == nu - 2:
                prev = st
                close(k - 1)
                continue
            mine = lax.all_gather(st, "vocab")
            grp = group_stats(pos, mine)
            *sent, grp = lax.optimization_barrier((*parts[k + 2], grp))
            stats[k] = (st, mine, send([grp])[0])
            recvs[k + 2] = send(sent)
            tok = grp
            if k >= 1:
                close(k - 1)
            peer(k + 3)
            mine_half(k + 2)
        return out, ct.reshape(rows_all)

    return jax.shard_map(
        pipeline,
        mesh=mesh,
        in_specs=(P("data", "hid"), P("hid", "vocab"), P("data"), P("data")),
        out_specs=(P("data", ("vocab", "hid")), P("data")),
        check_vma=False,
    )
```
